32 devices in a mesh: dp: 32 (over z, y, x, core), tensor: 1.
Axes of the slice: x: 2, y: 2, z: 4, core: 2. Of those that a mesh axis runs over, the one named last changes fastest.
Arguments:
- activations: bfloat16 [384, 8192], P('dp', 'tensor'), may hold values from -400 to 400, as said below
- weight: bfloat16 [8192, 28672], P('dp', 'tensor'), may hold values from -0.0625 to 0.0625
Outputs:
- channel_mean: float32 [8192], P('dp')
- column_errors: float32 [4, 28672], P(None, ('tensor', 'dp'))
- errors: float32 [4], replicated
The draws below stay inside these ranges and needn't reach their ends.
Inputs may be any that keep to these rules, and one draw needn't show every extreme that they name: activations and weight are finite real values within the ranges stated above.
All inputs are finite; a program needn't handle non-finite values.
Results may differ from the reference program's by a relative error of at most 0.0012.
The reference program's roundings to bfloat16 on the way (of `dequant`) count: a program that leaves them out, or rounds other values in their place, can miss the bound.
Values may be sent and summed in bfloat16 or wider, within the bound.
A program may use at most 128 MiB of HBM per device.

```python
import math
import jax
import jax.numpy as jnp
from jax import lax

D = 8192
F = 28672
GROUP = 128
GRID = 4
TOKENS = 384
N_TENSOR = 1


def draw_activations(key, part):
    base_key = jax.random.fold_in(key, 11)
    key_main, key_row, key_col = jax.random.split(base_key, 3)
    position = jnp.arange(TOKENS, dtype=jnp.float32) / max(TOKENS - 1, 1)
    row_scale = jnp.exp(math.log(4.0) * position + jax.random.uniform(key_row, (TOKENS,), jnp.float32, -0.3, 0.3))
    col_scale = jnp.exp(jax.random.uniform(key_col, (D,), jnp.float32, 0.0, math.log(10.0)))
    values = jnp.clip(jax.random.normal(key_main, (TOKENS, D), jnp.float32), -6.0, 6.0)
    return (values * row_scale[:, None] * col_scale[None, :]).astype(jnp.bfloat16)


def level_of(own_key, shape, cuts, smallest, top_value):
    gain, own = 1.0, jax.random.fold_in(own_key, 6)
    for axis_at, parts in cuts:
        draws = jnp.exp(jax.random.uniform(jax.random.fold_in(own, axis_at), (parts,), jnp.float32, smallest / len(cuts), top_value / len(cuts)))
        gain = gain * jnp.repeat(draws, shape[axis_at] // parts).reshape([-1 if axis == axis_at else 1 for axis in range(len(shape))])
    return gain


def scatter_about(stream_key, extent, spread, limit, cuts=(), kind=jnp.bfloat16):
    entries = spread * jax.random.normal(stream_key, extent, jnp.float32)
    if cuts:
        entries = entries * level_of(stream_key, extent, cuts, -0.22, 0.18)
    return jnp.clip(entries, -limit, limit).astype(kind)


def setup_inputs(seed: int = 0) -> dict:
    splits = jax.random.split(jax.random.key(seed), 3)
    return {
        "activations": draw_activations(jax.random.fold_in(splits[2], 71), 0),
        "weight": scatter_about(splits[1], (D, F), D ** -0.5, 0.0625, ((0, 32),)),
    }


def soft_round(values):
    return values - jnp.sin(2.0 * math.pi * values) / (2.0 * math.pi)

def scale_table(channel_mean):
    ratios = jnp.arange(GRID, dtype=jnp.float32) / GRID
    raw = jnp.exp(ratios[:, None] * jnp.log(channel_mean)[None, :])
    top = lax.optimization_barrier(jnp.max(raw, axis=1, keepdims=True))
    bottom = lax.optimization_barrier(jnp.min(raw, axis=1, keepdims=True))
    return raw / jnp.sqrt(top * bottom)

def block_errors(activations, block, scales):
    base_out = jnp.dot(activations, block, preferred_element_type=jnp.float32)
    width = block.shape[1]
    weight_float = block.astype(jnp.float32)

    def one_ratio(factor):
        scaled = weight_float * factor[:, None]
        grouped = scaled.reshape(D // GROUP, GROUP, width)
        quant_step = (lax.optimization_barrier(jnp.max(jnp.abs(grouped), axis=1, keepdims=True)) + 1e-06) / 7.0
        levels = soft_round(grouped / quant_step)
        dequant = ((levels * quant_step).reshape(D, width) / factor[:, None]).astype(jnp.bfloat16)
        quant_out = jnp.dot(activations, dequant, preferred_element_type=jnp.float32)
        residue = quant_out - base_out
        return lax.optimization_barrier(jnp.sum(residue * residue, axis=0))
    return lax.map(one_ratio, scales)

def reference(activations, weight):
    act_float = activations.astype(jnp.float32)
    channel_mean = lax.optimization_barrier(jnp.mean(jnp.abs(act_float), axis=0)) + 1e-06
    scales = scale_table(channel_mean)
    blocks = jnp.transpose(weight.reshape(D, N_TENSOR, F // N_TENSOR), (1, 0, 2))
    column_sums = lax.map(lambda block: block_errors(activations, block, scales), blocks)
    column_sums = jnp.transpose(column_sums, (1, 0, 2)).reshape(GRID, F)
    column_errors = column_sums / TOKENS
    errors = lax.optimization_barrier(jnp.sum(column_sums, axis=1)) / (TOKENS * F)
    return (channel_mean, column_errors, errors)
```

```python
import functools
import math

import jax
import jax.numpy as jnp
from jax import lax
from jax.experimental import pallas as pl
from jax.experimental.pallas import tpu as pltpu
from jax.sharding import PartitionSpec as P

GROUP = 128
GRID = 4
LANES = 128
TILE = 256
SINE = (
    6.283182818832115,
    -41.34142141640176,
    81.59618421926638,
    -76.5801034177733,
    41.205405703161745,
    -12.271277356143528,
)


def sine_of_turns(r):
    square = r * r
    value = SINE[-1] * square + SINE[-2]
    for c in SINE[-3::-1]:
        value = value * square + c
    return value * r


def partial_kernel(steps, a_ref, w_ref, s_ref, out_ref, acc, change):
    step = pl.program_id(0)
    depth, width = w_ref.shape

    @pl.when(step == 0)
    def _():
        acc[...] = jnp.zeros_like(acc)

    def tile(start, size):
        def columns(offset, length):
            if isinstance(start, int):
                return pl.ds(start + offset, length)
            return pl.ds(pl.multiple_of(start + offset, LANES), length)

        for k in range(GRID):
            for g in range(depth // GROUP):
                rows = pl.ds(g * GROUP, GROUP)
                for c in range(0, size, LANES):
                    lanes = min(LANES, size - c)
                    w = w_ref[rows, columns(c, lanes)].astype(jnp.float32)
                    scaled = w * s_ref[k, rows, :lanes]
                    top = jnp.max(jnp.abs(scaled), axis=0, keepdims=True)
                    quant_step = (top + 1e-06) / 7.0
                    v = scaled * (1.0 / quant_step)
                    wave = sine_of_turns(v - jnp.round(v))
                    wave = wave * (quant_step * (0.5 / math.pi))
                    dequant = w - wave * s_ref[GRID + k, rows, :lanes]
                    dequant = dequant.astype(jnp.bfloat16).astype(jnp.float32)
                    change[k, rows, pl.ds(c, lanes)] = (dequant - w).astype(jnp.bfloat16)
            acc[k, :, columns(0, size)] += jnp.dot(
                a_ref[...], change[k, :, pl.ds(0, size)], preferred_element_type=jnp.float32
            )

    whole = width // TILE
    if whole:

        @pl.loop(0, whole)
        def _(i):
            tile(i * TILE, TILE)

    if width % TILE:
        tile(whole * TILE, width % TILE)

    @pl.when(step == steps - 1)
    def _():
        for k in range(GRID):
            out_ref[k] = acc[k].astype(out_ref.dtype)


def partial_residue(tokens, columns, table, depth, kind):
    count, channels = tokens.shape
    width = columns.shape[1]
    steps = channels // depth
    return pl.pallas_call(
        functools.partial(partial_kernel, steps),
        grid=(steps,),
        out_shape=jax.ShapeDtypeStruct((GRID, count, width), kind),
        in_specs=[
            pl.BlockSpec((count, depth), lambda i: (0, i)),
            pl.BlockSpec((depth, width), lambda i: (i, 0)),
            pl.BlockSpec((2 * GRID, depth, LANES), lambda i: (0, i, 0)),
        ],
        out_specs=pl.BlockSpec((GRID, count, width), lambda i: (0, 0, 0)),
        scratch_shapes=[
            pltpu.VMEM((GRID, count, width), jnp.float32),
            pltpu.VMEM((GRID, depth, min(TILE, -(-width // LANES) * LANES)), jnp.bfloat16),
        ],
        compiler_params=pltpu.CompilerParams(
            dimension_semantics=("arbitrary",), vmem_limit_bytes=48 << 20
        ),
        cost_estimate=pl.CostEstimate(
            flops=30 * GRID * channels * width * 16,
            bytes_accessed=4 * channels * width,
            transcendentals=0,
        ),
    )(tokens, columns, table)


def in_halves(activations, weight):
    n = lax.axis_size("dp")
    half = n // 2
    me = lax.axis_index("dp")
    side, place = me // half, me % half
    groups = [list(range(half)), list(range(half, n))]
    across = [(i, (i + half) % n) for i in range(n)]

    widened = lax.all_gather(activations, "tensor", axis=1, tiled=True)
    own_tokens, channels = widened.shape
    mine = channels // 2
    token_count = own_tokens * n
    kept = lax.dynamic_slice_in_dim(widened, side * mine, mine, axis=1)
    away = lax.dynamic_slice_in_dim(widened, (1 - side) * mine, mine, axis=1)
    other = lax.ppermute(away, "dp", across)
    first = side == 0
    pair = jnp.concatenate([jnp.where(first, kept, other), jnp.where(first, other, kept)], axis=0)
    tokens = lax.all_gather(pair, "dp", axis=0, tiled=True, axis_index_groups=groups)

    width = weight.shape[1]
    away_weight = lax.dynamic_slice_in_dim(weight, (1 - side) * (width // 2), width // 2, axis=1)
    kept_weight = lax.dynamic_slice_in_dim(weight, side * (width // 2), width // 2, axis=1)
    exchange = functools.partial(
        lax.all_to_all, axis_name="dp", split_axis=1, concat_axis=0, tiled=True, axis_index_groups=groups
    )
    away_columns = exchange(away_weight)
    kept_columns = exchange(kept_weight)

    half_mean = jnp.sum(jnp.abs(tokens.astype(jnp.float32)), axis=0) / token_count + 1e-06
    other_mean = lax.ppermute(half_mean, "dp", across)
    ratios = jnp.arange(GRID, dtype=jnp.float32) / GRID
    raw = jnp.exp(ratios[:, None] * jnp.log(half_mean)[None, :])
    raw_other = jnp.exp(ratios[:, None] * jnp.log(other_mean)[None, :])
    top = jnp.maximum(jnp.max(raw, axis=1, keepdims=True), jnp.max(raw_other, axis=1, keepdims=True))
    bottom = jnp.minimum(jnp.min(raw, axis=1, keepdims=True), jnp.min(raw_other, axis=1, keepdims=True))
    scales = raw / jnp.sqrt(top * bottom)
    table = jnp.concatenate([scales, 1.0 / scales], axis=0)
    table = jnp.broadcast_to(table[:, :, None], (2 * GRID, mine, LANES))

    depth = weight.shape[0]
    away_part = partial_residue(tokens, away_columns, table, depth, jnp.bfloat16)
    arrived = lax.ppermute(away_part, "dp", across)
    own_part = partial_residue(tokens, kept_columns, table, depth, jnp.float32)
    residue = own_part + arrived.astype(jnp.float32)
    column_sums = jnp.sum(residue * residue, axis=1)

    totals = lax.psum(jnp.sum(column_sums, axis=1), ("dp", "tensor"))
    errors = totals / (token_count * width * lax.axis_size("tensor"))
    column_errors = column_sums / token_count
    own_mean = lax.dynamic_slice_in_dim(half_mean, place * depth, depth)
    return (own_mean, column_errors, errors)


PLANES = 4
CHUNK = 256
BLOCK = 512
AHEAD = 4
BOW = (12.568868617017895, 50.02489230906822, 77.93933755195671)
BOW_SHIFT = BOW[1] / (2.0 * BOW[2])
BOW_FLOOR = BOW[0] / BOW[2] - BOW_SHIFT * BOW_SHIFT


def change_of(w16, scale, unscale):
    w = w16.astype(jnp.float32)
    scaled = w if scale is None else w * scale
    top = jnp.max(jnp.abs(scaled), axis=0, keepdims=True) + 1e-06
    v = scaled * (7.0 / top)
    r = v - jnp.round(v)
    size = jnp.abs(r)
    rest = 0.5 - size
    m = size * rest + BOW_SHIFT
    wave = (r * rest) * (m * m + BOW_FLOOR) * (top * (BOW[2] / (14.0 * math.pi)))
    if unscale is not None:
        wave = wave * unscale
    return (w - wave).astype(jnp.bfloat16) - w16


def fused_kernel(
    n, a_ref, w_ref, mean_ref, col_ref, err_ref,
    wbuf, abuf, astage, table, meanrow, change, acc, stage, recv, colsum, cbuf, mine, theirs, etile, etiles,
    w_send, w_recv, az_send, az_recv, ab_send, ab_recv, mm_send, mm_recv, p_send, p_recv, c_send, c_recv, e_send, e_recv,
):
    depth = w_ref.shape[0]
    plane = n // PLANES
    channels = plane * depth
    chunks = wbuf.shape[0]
    half = chunks // 2
    tokens = abuf.shape[0]
    own = tokens // n
    rows_each = own * PLANES
    me = lax.axis_index("dp")
    z, p = me // plane, me % plane
    partner = p + 1 - 2 * (p % 2)

    def copy_to(device, source, target, send, arrive):
        return pltpu.make_async_remote_copy(
            src_ref=source, dst_ref=target, send_sem=send, recv_sem=arrive,
            device_id={"dp": device}, device_id_type=pl.DeviceIdType.MESH,
        )

    def settle(ref, sem):
        pltpu.make_async_copy(ref, ref, sem).wait()

    barrier = pltpu.get_barrier_semaphore()

    @pl.loop(1, n)
    def _(i):
        pl.semaphore_signal(
            barrier, inc=1, device_id={"dp": (me + i) % n}, device_id_type=pl.DeviceIdType.MESH
        )

    pl.semaphore_wait(barrier, n - 1)

    def slab(at):
        return a_ref.at[:, pl.ds(pl.multiple_of(at * channels, channels), channels)]

    def z_copy(i):
        to = (z + i) % PLANES
        return copy_to(to * plane + p, slab(to), astage.at[z], az_send.at[i], az_recv.at[z])

    for i in range(1, PLANES):
        z_copy(i).start()
    pltpu.make_async_copy(slab(z), astage.at[z], az_recv.at[z]).start()

    def chunk_of(step):
        return (step % 2) * half + step // 2

    def send_weights(step):
        c = chunk_of(step)
        rows = pl.ds(pl.multiple_of(p * depth, depth), depth)

        def piece(q):
            at = pl.multiple_of((q * chunks + c) * CHUNK, CHUNK)
            return w_ref.at[:, pl.ds(at, CHUNK)]

        @pl.loop(1, plane)
        def _(j):
            q = (p + j) % plane
            copy_to(z * plane + q, piece(q), wbuf.at[c, rows, :], w_send.at[c], w_recv.at[c]).start()

        pltpu.make_async_copy(piece(p), wbuf.at[c, rows, :], w_recv.at[c]).start()

    send_weights(0)

    for i in range(PLANES):
        settle(astage.at[i], az_recv.at[i])

    def block(q):
        return abuf.at[pl.ds(pl.multiple_of(q * rows_each, rows_each), rows_each), :]

    @pl.loop(0, channels // LANES)
    def _(i):
        lanes = pl.ds(pl.multiple_of(i * LANES, LANES), LANES)
        part = [astage[t, :, lanes].astype(jnp.float32)[:own] for t in range(PLANES)]
        whole = jnp.concatenate(part, axis=0).astype(jnp.bfloat16)
        abuf[pl.ds(pl.multiple_of(p * rows_each, rows_each), rows_each), lanes] = whole

    for j in range(1, plane // 2):
        to = (p + 2 * j) % plane
        copy_to(z * plane + to, block(p), block(p), ab_send.at[j], ab_recv.at[p]).start()
    copy_to(z * plane + partner, block(p), block(p), ab_send.at[0], ab_recv.at[p]).start()

    for step in range(1, AHEAD):
        send_weights(step)

    for j in range(1, plane // 2):
        q = (p + 2 * j) % plane
        settle(block(q), ab_recv.at[q])
        copy_to(z * plane + partner, block(q), block(q), ab_send.at[plane // 2 + j - 1], ab_recv.at[q]).start()
    for j in range(plane // 2):
        q = (partner + 2 * j) % plane
        settle(block(q), ab_recv.at[q])

    def means(i, carry):
        most, least = carry
        lanes = pl.ds(pl.multiple_of(i * LANES, LANES), LANES)
        sums = jnp.sum(jnp.abs(abuf[:, lanes].astype(jnp.float32)), axis=0, keepdims=True)
        mean = sums / tokens + 1e-06
        meanrow[:, lanes] = mean
        table[0, lanes, :] = jnp.transpose(jnp.broadcast_to(jnp.log(mean), (LANES, LANES)))
        return jnp.maximum(most, mean), jnp.minimum(least, mean)

    most, least = lax.fori_loop(
        0, channels // LANES, means,
        (jnp.zeros((1, LANES), jnp.float32), jnp.full((1, LANES), jnp.inf, jnp.float32)),
    )
    mean_ref[...] = meanrow[:, pl.ds(pl.multiple_of(p * depth, depth), depth)]
    mine[0:1, :] = most
    mine[1:2, :] = least

    def mm_copy(i):
        to = (z + i) % PLANES
        return copy_to(to * plane + p, mine, theirs.at[i], mm_send.at[i], mm_recv.at[i])

    for i in range(1, PLANES):
        mm_copy(i).start()
    for i in range(1, PLANES):
        settle(theirs.at[i], mm_recv.at[i])
        most = jnp.maximum(most, theirs[i, 0:1, :])
        least = jnp.minimum(least, theirs[i, 1:2, :])
    ends = jnp.log(jnp.max(most, axis=1, keepdims=True)) + jnp.log(jnp.min(least, axis=1, keepdims=True))
    middle = 0.5 * ends

    @pl.loop(0, channels // LANES)
    def _(i):
        rows = pl.ds(pl.multiple_of(i * LANES, LANES), LANES)
        level = table[0, rows, :] - middle
        for k in range(1, GRID):
            table[2 * k - 2, rows, :] = jnp.exp((k / GRID) * level)
            table[2 * k - 1, rows, :] = jnp.exp((-k / GRID) * level)

    def partial_products(c):
        acc[...] = jnp.zeros_like(acc)

        @pl.loop(0, channels // BLOCK)
        def _(b):
            base = pl.multiple_of(b * BLOCK, BLOCK)
            lhs = abuf[:, pl.ds(base, BLOCK)]
            for k in range(GRID):
                for g in range(BLOCK // GROUP):
                    rows = pl.ds(base + g * GROUP, GROUP)
                    for h in range(0, CHUNK, LANES):
                        w16 = wbuf[c, rows, pl.ds(h, LANES)]
                        scale = table[2 * k - 2, rows, :] if k else None
                        unscale = table[2 * k - 1, rows, :] if k else None
                        change[k, pl.ds(g * GROUP, GROUP), pl.ds(h, LANES)] = change_of(w16, scale, unscale)
                acc[k] += jnp.dot(lhs, change[k], preferred_element_type=jnp.float32)

    def hand_on(c, k, to):
        return copy_to(to * plane + p, stage.at[c, k], recv.at[c, k], p_send.at[c, k], p_recv.at[c, k])

    steps = chunks
    for_side = ((PLANES - 1 - z, z - 1), (z, z + 1))

    @pl.loop(0, steps + PLANES - 1)
    def _(step):
        @pl.when(step < steps)
        def _():
            c = chunk_of(step)

            @pl.when(step + AHEAD < steps)
            def _():
                send_weights(step + AHEAD)

            settle(wbuf.at[c], w_recv.at[c])
            partial_products(c)
            for k in range(GRID):
                stage[c, k] = acc[k].astype(jnp.bfloat16)
            for side in range(2):
                gone, to = for_side[side]

                @pl.when((step % 2 == side) & (gone == 0))
                def _():
                    for k in range(GRID):
                        hand_on(c, k, to).start()

        for side in range(2):
            gone, to = for_side[side]
            late = step - gone
            c = side * half + (late + 2) // 2 - 1
            ready = (gone > 0) & (late >= 0) & (late < steps) & ((late + 2) % 2 == side)

            @pl.when(ready & (gone < PLANES - 1))
            def _():
                for k in range(GRID):
                    settle(recv.at[c, k], p_recv.at[c, k])
                    total = stage[c, k].astype(jnp.float32) + recv[c, k].astype(jnp.float32)
                    stage[c, k] = total.astype(jnp.bfloat16)
                    hand_on(c, k, to).start()

            @pl.when(ready & (gone == PLANES - 1))
            def _():
                for k in range(GRID):
                    settle(recv.at[c, k], p_recv.at[c, k])
                    residue = stage[c, k].astype(jnp.float32) + recv[c, k].astype(jnp.float32)
                    sums = jnp.sum(residue * residue, axis=0, keepdims=True)
                    for h in range(0, CHUNK, LANES):
                        at = c * CHUNK + h
                        width = colsum.shape[2]
                        lanes = pl.ds(pl.multiple_of(at % width, LANES), LANES)
                        colsum[at // width, k : k + 1, lanes] = sums[:, h : h + LANES]

    finishing = (z == 0) | (z == PLANES - 1)
    first_block = jnp.where(z == 0, 0, PLANES // 2)
    slot = jnp.where(z == 0, p, plane + p)

    def column_copy(i):
        j = first_block + i
        return copy_to(p * PLANES + j, colsum.at[j], cbuf, c_send.at[i], c_recv)

    def total_copy(i):
        return copy_to((me + i) % n, etile, etiles.at[slot], e_send.at[i], e_recv.at[slot])

    @pl.when(finishing)
    def _():
        for i in range(PLANES // 2):
            to_self = p * PLANES + first_block + i == me

            @pl.when(jnp.logical_not(to_self))
            def _():
                column_copy(i).start()

            @pl.when(to_self)
            def _():
                cbuf[...] = colsum[first_block + i]

        total = jnp.zeros((8, 1), jnp.float32)
        for i in range(PLANES // 2):
            total += jnp.sum(colsum[first_block + i], axis=1, keepdims=True)
        etile[...] = jnp.broadcast_to(total, (8, LANES))
        etiles[slot] = etile[...]

        @pl.loop(1, n)
        def _(i):
            total_copy(i).start()

    block_from, block_at = me // PLANES, me % PLANES
    source = jnp.where(block_at < PLANES // 2, 0, PLANES - 1) * plane + block_from

    @pl.when(source != me)
    def _():
        settle(cbuf, c_recv)

    col_ref[...] = cbuf[...] * (1.0 / tokens)

    @pl.loop(0, 2 * plane)
    def _(i):
        @pl.when(jnp.logical_not(finishing & (i == slot)))
        def _():
            settle(etiles.at[i], e_recv.at[i])

    total = jnp.zeros((8, LANES), jnp.float32)
    for i in range(2 * plane):
        total += etiles[i]
    err_ref[...] = total * (1.0 / (tokens * plane * chunks * CHUNK))

    for i in range(1, PLANES):
        z_copy(i).wait_send()
        mm_copy(i).wait_send()
    for i in range(plane - 1):
        settle(block(0), ab_send.at[i])

    @pl.loop(0, chunks)
    def _(c):
        settle(wbuf.at[0, pl.ds(0, channels - depth), :], w_send.at[c])

        for side in range(2):
            gone, to = for_side[side]

            @pl.when((c // half == side) & (gone < PLANES - 1))
            def _():
                for k in range(GRID):
                    settle(stage.at[c, k], p_send.at[c, k])

    @pl.when(finishing)
    def _():
        for i in range(PLANES // 2):

            @pl.when(p * PLANES + first_block + i != me)
            def _():
                settle(colsum.at[0], c_send.at[i])

        @pl.loop(1, n)
        def _(i):
            settle(etile, e_send.at[i])


def in_one_kernel(activations, weight):
    n = lax.axis_size("dp")
    own, depth = activations.shape[0], weight.shape[0]
    plane = n // PLANES
    channels, tokens = plane * depth, n * own
    chunks = weight.shape[1] // (plane * CHUNK)
    width = weight.shape[1] // n
    padded = -(-own // 16) * 16
    activations = jnp.pad(activations, ((0, padded - own), (0, 0)))
    dma, f32, bf16 = pltpu.SemaphoreType.DMA, jnp.float32, jnp.bfloat16
    mean, columns, errors = pl.pallas_call(
        functools.partial(fused_kernel, n),
        out_shape=(
            jax.ShapeDtypeStruct((1, depth), f32),
            jax.ShapeDtypeStruct((8, width), f32),
            jax.ShapeDtypeStruct((8, LANES), f32),
        ),
        in_specs=[pl.BlockSpec(memory_space=pl.ANY)] * 2,
        out_specs=[pl.BlockSpec(memory_space=pltpu.VMEM)] * 3,
        scratch_shapes=[
            pltpu.VMEM((chunks, channels, CHUNK), bf16),
            pltpu.VMEM((tokens, channels), bf16),
            pltpu.VMEM((PLANES, padded, channels), bf16),
            pltpu.VMEM((2 * GRID - 2, channels, LANES), f32),
            pltpu.VMEM((1, channels), f32),
            pltpu.VMEM((GRID, BLOCK, CHUNK), bf16),
            pltpu.VMEM((GRID, tokens, CHUNK), f32),
            pltpu.VMEM((chunks, GRID, tokens, CHUNK), bf16),
            pltpu.VMEM((chunks, GRID, tokens, CHUNK), bf16),
            pltpu.VMEM((PLANES, 8, width), f32),
            pltpu.VMEM((8, width), f32),
            pltpu.VMEM((8, LANES), f32),
            pltpu.VMEM((PLANES, 8, LANES), f32),
            pltpu.VMEM((8, LANES), f32),
            pltpu.VMEM((2 * plane, 8, LANES), f32),
            dma((chunks,)), dma((chunks,)),
            dma((PLANES,)), dma((PLANES,)),
            dma((plane,)), dma((plane,)),
            dma((PLANES,)), dma((PLANES,)),
            dma((chunks, GRID)), dma((chunks, GRID)),
            dma((PLANES // 2,)), dma,
            dma((n,)), dma((2 * plane,)),
        ],
        compiler_params=pltpu.CompilerParams(
            collective_id=0, has_side_effects=True, vmem_limit_bytes=62 << 20
        ),
    )(activations, weight)
    return (mean.reshape(depth), columns[:GRID], errors[:GRID, 0])


def one_kernel_fits(activations, weight):
    n, tensor = lax.axis_size("dp"), lax.axis_size("tensor")
    if tensor != 1 or n % (2 * PLANES) or n < 4 * PLANES:
        return False
    plane = n // PLANES
    channels, width = plane * weight.shape[0], weight.shape[1]
    aligned = (activations.shape[0] * PLANES) % 16 == 0 and weight.shape[0] % GROUP == 0
    return aligned and channels % BLOCK == 0 and width % (2 * CHUNK * plane) == 0 and width % (LANES * n) == 0


def on_device(activations, weight):
    if one_kernel_fits(activations, weight):
        return in_one_kernel(activations, weight)
    return in_halves(activations, weight)


def solution(mesh):
    placed = (P("dp", "tensor"), P("dp", "tensor"))
    return jax.shard_map(
        on_device,
        mesh=mesh,
        in_specs=placed,
        out_specs=(P("dp"), P(None, ("tensor", "dp")), P()),
        check_vma=False,
    )
```

```python
import functools
import math

import jax
import jax.numpy as jnp
from jax import lax
from jax.experimental import pallas as pl
from jax.experimental.pallas import tpu as pltpu
from jax.sharding import PartitionSpec as P

GROUP = 128
GRID = 4
LANES = 128
TILE = 256
SINE = (
    6.283182818832115,
    -41.34142141640176,
    81.59618421926638,
    -76.5801034177733,
    41.205405703161745,
    -12.271277356143528,
)


def sine_of_turns(r):
    square = r * r
    value = SINE[-1] * square + SINE[-2]
    for c in SINE[-3::-1]:
        value = value * square + c
    return value * r


def partial_kernel(steps, a_ref, w_ref, s_ref, out_ref, acc, change):
    step = pl.program_id(0)
    depth, width = w_ref.shape

    @pl.when(step == 0)
    def _():
        acc[...] = jnp.zeros_like(acc)

    def tile(start, size):
        def columns(offset, length):
            if isinstance(start, int):
                return pl.ds(start + offset, length)
            return pl.ds(pl.multiple_of(start + offset, LANES), length)

        for k in range(GRID):
            for g in range(depth // GROUP):
                rows = pl.ds(g * GROUP, GROUP)
                for c in range(0, size, LANES):
                    lanes = min(LANES, size - c)
                    w = w_ref[rows, columns(c, lanes)].astype(jnp.float32)
                    scaled = w * s_ref[k, rows, :lanes]
                    top = jnp.max(jnp.abs(scaled), axis=0, keepdims=True)
                    quant_step = (top + 1e-06) / 7.0
                    v = scaled * (1.0 / quant_step)
                    wave = sine_of_turns(v - jnp.round(v))
                    wave = wave * (quant_step * (0.5 / math.pi))
                    dequant = w - wave * s_ref[GRID + k, rows, :lanes]
                    dequant = dequant.astype(jnp.bfloat16).astype(jnp.float32)
                    change[k, rows, pl.ds(c, lanes)] = (dequant - w).astype(jnp.bfloat16)
            acc[k, :, columns(0, size)] += jnp.dot(
                a_ref[...], change[k, :, pl.ds(0, size)], preferred_element_type=jnp.float32
            )

    whole = width // TILE
    if whole:

        @pl.loop(0, whole)
        def _(i):
            tile(i * TILE, TILE)

    if width % TILE:
        tile(whole * TILE, width % TILE)

    @pl.when(step == steps - 1)
    def _():
        for k in range(GRID):
            out_ref[k] = acc[k].astype(out_ref.dtype)


def partial_residue(tokens, columns, table, depth, kind):
    count, channels = tokens.shape
    width = columns.shape[1]
    steps = channels // depth
    return pl.pallas_call(
        functools.partial(partial_kernel, steps),
        grid=(steps,),
        out_shape=jax.ShapeDtypeStruct((GRID, count, width), kind),
        in_specs=[
            pl.BlockSpec((count, depth), lambda i: (0, i)),
            pl.BlockSpec((depth, width), lambda i: (i, 0)),
            pl.BlockSpec((2 * GRID, depth, LANES), lambda i: (0, i, 0)),
        ],
        out_specs=pl.BlockSpec((GRID, count, width), lambda i: (0, 0, 0)),
        scratch_shapes=[
            pltpu.VMEM((GRID, count, width), jnp.float32),
            pltpu.VMEM((GRID, depth, min(TILE, -(-width // LANES) * LANES)), jnp.bfloat16),
        ],
        compiler_params=pltpu.CompilerParams(
            dimension_semantics=("arbitrary",), vmem_limit_bytes=48 << 20
        ),
        cost_estimate=pl.CostEstimate(
            flops=30 * GRID * channels * width * 16,
            bytes_accessed=4 * channels * width,
            transcendentals=0,
        ),
    )(tokens, columns, table)


def in_halves(activations, weight):
    n = lax.axis_size("dp")
    half = n // 2
    me = lax.axis_index("dp")
    side, place = me // half, me % half
    groups = [list(range(half)), list(range(half, n))]
    across = [(i, (i + half) % n) for i in range(n)]

    widened = lax.all_gather(activations, "tensor", axis=1, tiled=True)
    own_tokens, channels = widened.shape
    mine = channels // 2
    token_count = own_tokens * n
    kept = lax.dynamic_slice_in_dim(widened, side * mine, mine, axis=1)
    away = lax.dynamic_slice_in_dim(widened, (1 - side) * mine, mine, axis=1)
    other = lax.ppermute(away, "dp", across)
    first = side == 0
    pair = jnp.concatenate([jnp.where(first, kept, other), jnp.where(first, other, kept)], axis=0)
    tokens = lax.all_gather(pair, "dp", axis=0, tiled=True, axis_index_groups=groups)

    width = weight.shape[1]
    away_weight = lax.dynamic_slice_in_dim(weight, (1 - side) * (width // 2), width // 2, axis=1)
    kept_weight = lax.dynamic_slice_in_dim(weight, side * (width // 2), width // 2, axis=1)
    exchange = functools.partial(
        lax.all_to_all, axis_name="dp", split_axis=1, concat_axis=0, tiled=True, axis_index_groups=groups
    )
    away_columns = exchange(away_weight)
    kept_columns = exchange(kept_weight)

    half_mean = jnp.sum(jnp.abs(tokens.astype(jnp.float32)), axis=0) / token_count + 1e-06
    other_mean = lax.ppermute(half_mean, "dp", across)
    ratios = jnp.arange(GRID, dtype=jnp.float32) / GRID
    raw = jnp.exp(ratios[:, None] * jnp.log(half_mean)[None, :])
    raw_other = jnp.exp(ratios[:, None] * jnp.log(other_mean)[None, :])
    top = jnp.maximum(jnp.max(raw, axis=1, keepdims=True), jnp.max(raw_other, axis=1, keepdims=True))
    bottom = jnp.minimum(jnp.min(raw, axis=1, keepdims=True), jnp.min(raw_other, axis=1, keepdims=True))
    scales = raw / jnp.sqrt(top * bottom)
    table = jnp.concatenate([scales, 1.0 / scales], axis=0)
    table = jnp.broadcast_to(table[:, :, None], (2 * GRID, mine, LANES))

    depth = weight.shape[0]
    away_part = partial_residue(tokens, away_columns, table, depth, jnp.bfloat16)
    arrived = lax.ppermute(away_part, "dp", across)
    own_part = partial_residue(tokens, kept_columns, table, depth, jnp.float32)
    residue = own_part + arrived.astype(jnp.float32)
    column_sums = jnp.sum(residue * residue, axis=1)

    totals = lax.psum(jnp.sum(column_sums, axis=1), ("dp", "tensor"))
    errors = totals / (token_count * width * lax.axis_size("tensor"))
    column_errors = column_sums / token_count
    own_mean = lax.dynamic_slice_in_dim(half_mean, place * depth, depth)
    return (own_mean, column_errors, errors)


PLANES = 4
CHUNK = 128
BLOCK = 512
AHEAD = 4
LAG = 2
BOW = (12.568868617017895, 50.02489230906822, 77.93933755195671)
BOW_SHIFT = BOW[1] / (2.0 * BOW[2])
BOW_FLOOR = BOW[0] / BOW[2] - BOW_SHIFT * BOW_SHIFT


def change_of(w16, scale, unscale):
    w = w16.astype(jnp.float32)
    scaled = w if scale is None else w * scale
    top = jnp.max(jnp.abs(scaled), axis=0, keepdims=True) + 1e-06
    v = scaled * (7.0 / top)
    r = v - jnp.round(v)
    size = jnp.abs(r)
    rest = 0.5 - size
    m = size * rest + BOW_SHIFT
    wave = (r * rest) * (m * m + BOW_FLOOR) * (top * (BOW[2] / (14.0 * math.pi)))
    if unscale is not None:
        wave = wave * unscale
    return (w - wave).astype(jnp.bfloat16) - w16


def fused_kernel(
    n, a_ref, w_ref, mean_ref, col_ref, err_ref,
    wbuf, abuf, astage, table, meanrow, change, acc, stage, recv, colsum, cbuf, mine, theirs, etile, etiles,
    w_send, w_recv, az_send, az_recv, ab_send, ab_recv, mm_send, mm_recv, p_send, p_recv, c_send, c_recv, e_send, e_recv,
):
    depth = w_ref.shape[0]
    plane = n // PLANES
    channels = plane * depth
    chunks = wbuf.shape[0]
    half = chunks // 2
    tokens = abuf.shape[0]
    own = tokens // n
    rows_each = own * PLANES
    me = lax.axis_index("dp")
    z, p = me // plane, me % plane
    partner = p + 1 - 2 * (p % 2)

    def copy_to(device, source, target, send, arrive):
        return pltpu.make_async_remote_copy(
            src_ref=source, dst_ref=target, send_sem=send, recv_sem=arrive,
            device_id={"dp": device}, device_id_type=pl.DeviceIdType.MESH,
        )

    def settle(ref, sem):
        pltpu.make_async_copy(ref, ref, sem).wait()

    barrier = pltpu.get_barrier_semaphore()

    @pl.loop(1, n)
    def _(i):
        pl.semaphore_signal(
            barrier, inc=1, device_id={"dp": (me + i) % n}, device_id_type=pl.DeviceIdType.MESH
        )

    pl.semaphore_wait(barrier, n - 1)

    def slab(at):
        return a_ref.at[:, pl.ds(pl.multiple_of(at * channels, channels), channels)]

    def z_copy(i):
        to = (z + i) % PLANES
        return copy_to(to * plane + p, slab(to), astage.at[z], az_send.at[i], az_recv.at[z])

    for i in range(1, PLANES):
        z_copy(i).start()
    pltpu.make_async_copy(slab(z), astage.at[z], az_recv.at[z]).start()

    def chunk_of(step):
        return (step % 2) * half + step // 2

    def send_weights(step):
        c = chunk_of(step)
        rows = pl.ds(pl.multiple_of(p * depth, depth), depth)

        def piece(q):
            at = pl.multiple_of((q * chunks + c) * CHUNK, CHUNK)
            return w_ref.at[:, pl.ds(at, CHUNK)]

        @pl.loop(1, plane)
        def _(j):
            q = (p + j) % plane
            copy_to(z * plane + q, piece(q), wbuf.at[c, rows, :], w_send.at[c], w_recv.at[c]).start()

        pltpu.make_async_copy(piece(p), wbuf.at[c, rows, :], w_recv.at[c]).start()

    send_weights(0)

    for i in range(PLANES):
        settle(astage.at[i], az_recv.at[i])

    def block(q):
        return abuf.at[pl.ds(pl.multiple_of(q * rows_each, rows_each), rows_each), :]

    @pl.loop(0, channels // LANES)
    def _(i):
        lanes = pl.ds(pl.multiple_of(i * LANES, LANES), LANES)
        part = [astage[t, :, lanes].astype(jnp.float32) for t in range(PLANES)]
        whole = jnp.concatenate(part, axis=0).astype(jnp.bfloat16)
        abuf[pl.ds(pl.multiple_of(p * rows_each, rows_each), rows_each), lanes] = whole

    for j in range(1, plane // 2):
        to = (p + 2 * j) % plane
        copy_to(z * plane + to, block(p), block(p), ab_send.at[j], ab_recv.at[p]).start()
    copy_to(z * plane + partner, block(p), block(p), ab_send.at[0], ab_recv.at[p]).start()

    for step in range(1, AHEAD):
        send_weights(step)

    for j in range(1, plane // 2):
        q = (p + 2 * j) % plane
        settle(block(q), ab_recv.at[q])
        copy_to(z * plane + partner, block(q), block(q), ab_send.at[plane // 2 + j - 1], ab_recv.at[q]).start()
    for j in range(plane // 2):
        q = (partner + 2 * j) % plane
        settle(block(q), ab_recv.at[q])

    def means(i, carry):
        most, least = carry
        lanes = pl.ds(pl.multiple_of(i * LANES, LANES), LANES)
        sums = jnp.sum(jnp.abs(abuf[:, lanes].astype(jnp.float32)), axis=0, keepdims=True)
        mean = sums / tokens + 1e-06
        meanrow[:, lanes] = mean
        table[0, lanes, :] = jnp.transpose(jnp.broadcast_to(jnp.log(mean), (LANES, LANES)))
        return jnp.maximum(most, mean), jnp.minimum(least, mean)

    most, least = lax.fori_loop(
        0, channels // LANES, means,
        (jnp.zeros((1, LANES), jnp.float32), jnp.full((1, LANES), jnp.inf, jnp.float32)),
    )
    mean_ref[...] = meanrow[:, pl.ds(pl.multiple_of(p * depth, depth), depth)]
    mine[0:1, :] = most
    mine[1:2, :] = least

    def mm_copy(i):
        to = (z + i) % PLANES
        return copy_to(to * plane + p, mine, theirs.at[i], mm_send.at[i], mm_recv.at[i])

    for i in range(1, PLANES):
        mm_copy(i).start()
    for i in range(1, PLANES):
        settle(theirs.at[i], mm_recv.at[i])
        most = jnp.maximum(most, theirs[i, 0:1, :])
        least = jnp.minimum(least, theirs[i, 1:2, :])
    ends = jnp.log(jnp.max(most, axis=1, keepdims=True)) + jnp.log(jnp.min(least, axis=1, keepdims=True))
    middle = 0.5 * ends

    @pl.loop(0, channels // LANES)
    def _(i):
        rows = pl.ds(pl.multiple_of(i * LANES, LANES), LANES)
        level = table[0, rows, :] - middle
        for k in range(1, GRID):
            table[2 * k - 2, rows, :] = jnp.exp((k / GRID) * level)
            table[2 * k - 1, rows, :] = jnp.exp((-k / GRID) * level)

    def partial_products(c):
        acc[...] = jnp.zeros_like(acc)

        @pl.loop(0, channels // BLOCK)
        def _(b):
            base = pl.multiple_of(b * BLOCK, BLOCK)
            lhs = abuf[:, pl.ds(base, BLOCK)]
            for k in range(GRID):
                for g in range(BLOCK // GROUP):
                    rows = pl.ds(base + g * GROUP, GROUP)
                    for h in range(0, CHUNK, LANES):
                        w16 = wbuf[c, rows, pl.ds(h, LANES)]
                        scale = table[2 * k - 2, rows, :] if k else None
                        unscale = table[2 * k - 1, rows, :] if k else None
                        change[k, pl.ds(g * GROUP, GROUP), pl.ds(h, LANES)] = change_of(w16, scale, unscale)
                acc[k] += jnp.dot(lhs, change[k], preferred_element_type=jnp.float32)

    def hand_on(c, k, to):
        return copy_to(to * plane + p, stage.at[c, k], recv.at[c, k], p_send.at[c, k], p_recv.at[c, k])

    steps = chunks
    for_side = ((PLANES - 1 - z, z - 1), (z, z + 1))

    @pl.loop(0, steps + LAG * (PLANES - 1))
    def _(step):
        @pl.when(step < steps)
        def _():
            c = chunk_of(step)

            @pl.when(step + AHEAD < steps)
            def _():
                send_weights(step + AHEAD)

            settle(wbuf.at[c], w_recv.at[c])
            partial_products(c)
            for k in range(GRID):
                stage[c, k] = acc[k].astype(jnp.bfloat16)
            for side in range(2):
                gone, to = for_side[side]

                @pl.when((step % 2 == side) & (gone == 0))
                def _():
                    for k in range(GRID):
                        hand_on(c, k, to).start()

        for side in range(2):
            gone, to = for_side[side]
            late = step - LAG * gone
            c = side * half + late // 2
            ready = (gone > 0) & (late >= 0) & (late < steps) & (step % 2 == side)

            @pl.when(ready & (gone < PLANES - 1))
            def _():
                for k in range(GRID):
                    settle(recv.at[c, k], p_recv.at[c, k])
                    total = stage[c, k].astype(jnp.float32) + recv[c, k].astype(jnp.float32)
                    stage[c, k] = total.astype(jnp.bfloat16)
                    hand_on(c, k, to).start()

            @pl.when(ready & (gone == PLANES - 1))
            def _():
                for k in range(GRID):
                    settle(recv.at[c, k], p_recv.at[c, k])
                    residue = stage[c, k].astype(jnp.float32) + recv[c, k].astype(jnp.float32)
                    sums = jnp.sum(residue * residue, axis=0, keepdims=True)
                    for h in range(0, CHUNK, LANES):
                        at = c * CHUNK + h
                        width = colsum.shape[2]
                        lanes = pl.ds(pl.multiple_of(at % width, LANES), LANES)
                        colsum[at // width, k : k + 1, lanes] = sums[:, h : h + LANES]

    finishing = (z == 0) | (z == PLANES - 1)
    first_block = jnp.where(z == 0, 0, PLANES // 2)
    slot = jnp.where(z == 0, p, plane + p)

    def column_copy(i):
        j = first_block + i
        return copy_to(p * PLANES + j, colsum.at[j], cbuf, c_send.at[i], c_recv)

    def total_copy(i):
        return copy_to((me + i) % n, etile, etiles.at[slot], e_send.at[i], e_recv.at[slot])

    @pl.when(finishing)
    def _():
        for i in range(PLANES // 2):
            to_self = p * PLANES + first_block + i == me

            @pl.when(jnp.logical_not(to_self))
            def _():
                column_copy(i).start()

            @pl.when(to_self)
            def _():
                cbuf[...] = colsum[first_block + i]

        total = jnp.zeros((8, 1), jnp.float32)
        for i in range(PLANES // 2):
            total += jnp.sum(colsum[first_block + i], axis=1, keepdims=True)
        etile[...] = jnp.broadcast_to(total, (8, LANES))
        etiles[slot] = etile[...]

        @pl.loop(1, n)
        def _(i):
            total_copy(i).start()

    block_from, block_at = me // PLANES, me % PLANES
    source = jnp.where(block_at < PLANES // 2, 0, PLANES - 1) * plane + block_from

    @pl.when(source != me)
    def _():
        settle(cbuf, c_recv)

    col_ref[...] = cbuf[...] * (1.0 / tokens)

    @pl.loop(0, 2 * plane)
    def _(i):
        @pl.when(jnp.logical_not(finishing & (i == slot)))
        def _():
            settle(etiles.at[i], e_recv.at[i])

    total = jnp.zeros((8, LANES), jnp.float32)
    for i in range(2 * plane):
        total += etiles[i]
    err_ref[...] = total * (1.0 / (tokens * plane * chunks * CHUNK))

    for i in range(1, PLANES):
        z_copy(i).wait_send()
        mm_copy(i).wait_send()
    for i in range(plane - 1):
        settle(block(0), ab_send.at[i])

    @pl.loop(0, chunks)
    def _(c):
        settle(wbuf.at[0, pl.ds(0, channels - depth), :], w_send.at[c])

        for side in range(2):
            gone, to = for_side[side]

            @pl.when((c // half == side) & (gone < PLANES - 1))
            def _():
                for k in range(GRID):
                    settle(stage.at[c, k], p_send.at[c, k])

    @pl.when(finishing)
    def _():
        for i in range(PLANES // 2):

            @pl.when(p * PLANES + first_block + i != me)
            def _():
                settle(colsum.at[0], c_send.at[i])

        @pl.loop(1, n)
        def _(i):
            settle(etile, e_send.at[i])


def in_one_kernel(activations, weight):
    n = lax.axis_size("dp")
    own, depth = activations.shape[0], weight.shape[0]
    plane = n // PLANES
    channels, tokens = plane * depth, n * own
    chunks = weight.shape[1] // (plane * CHUNK)
    width = weight.shape[1] // n
    dma, f32, bf16 = pltpu.SemaphoreType.DMA, jnp.float32, jnp.bfloat16
    mean, columns, errors = pl.pallas_call(
        functools.partial(fused_kernel, n),
        out_shape=(
            jax.ShapeDtypeStruct((1, depth), f32),
            jax.ShapeDtypeStruct((8, width), f32),
            jax.ShapeDtypeStruct((8, LANES), f32),
        ),
        in_specs=[pl.BlockSpec(memory_space=pl.ANY)] * 2,
        out_specs=[pl.BlockSpec(memory_space=pltpu.VMEM)] * 3,
        scratch_shapes=[
            pltpu.VMEM((chunks, channels, CHUNK), bf16),
            pltpu.VMEM((tokens, channels), bf16),
            pltpu.VMEM((PLANES, own, channels), bf16),
            pltpu.VMEM((2 * GRID - 2, channels, LANES), f32),
            pltpu.VMEM((1, channels), f32),
            pltpu.VMEM((GRID, BLOCK, CHUNK), bf16),
            pltpu.VMEM((GRID, tokens, CHUNK), f32),
            pltpu.VMEM((chunks, GRID, tokens, CHUNK), bf16),
            pltpu.VMEM((chunks, GRID, tokens, CHUNK), bf16),
            pltpu.VMEM((PLANES, 8, width), f32),
            pltpu.VMEM((8, width), f32),
            pltpu.VMEM((8, LANES), f32),
            pltpu.VMEM((PLANES, 8, LANES), f32),
            pltpu.VMEM((8, LANES), f32),
            pltpu.VMEM((2 * plane, 8, LANES), f32),
            dma((chunks,)), dma((chunks,)),
            dma((PLANES,)), dma((PLANES,)),
            dma((plane,)), dma((plane,)),
            dma((PLANES,)), dma((PLANES,)),
            dma((chunks, GRID)), dma((chunks, GRID)),
            dma((PLANES // 2,)), dma,
            dma((n,)), dma((2 * plane,)),
        ],
        compiler_params=pltpu.CompilerParams(
            collective_id=0, has_side_effects=True, vmem_limit_bytes=62 << 20
        ),
    )(activations, weight)
    return (mean.reshape(depth), columns[:GRID], errors[:GRID, 0])


def one_kernel_fits(activations, weight):
    n, tensor = lax.axis_size("dp"), lax.axis_size("tensor")
    if tensor != 1 or n % (2 * PLANES) or n < 4 * PLANES:
        return False
    plane = n // PLANES
    channels, width = plane * weight.shape[0], weight.shape[1]
    aligned = (activations.shape[0] * PLANES) % 16 == 0 and weight.shape[0] % GROUP == 0
    return aligned and channels % BLOCK == 0 and width % (2 * CHUNK * plane) == 0 and width % (LANES * n) == 0


def on_device(activations, weight):
    if one_kernel_fits(activations, weight):
        return in_one_kernel(activations, weight)
    return in_halves(activations, weight)


def solution(mesh):
    placed = (P("dp", "tensor"), P("dp", "tensor"))
    return jax.shard_map(
        on_device,
        mesh=mesh,
        in_specs=placed,
        out_specs=(P("dp"), P(None, ("tensor", "dp")), P()),
        check_vma=False,
    )
```

```python
import functools
import math

import jax
import jax.numpy as jnp
from jax import lax
from jax.experimental import pallas as pl
from jax.experimental.pallas import tpu as pltpu
from jax.sharding import PartitionSpec as P

GROUP = 128
GRID = 4
LANES = 128
TILE = 256
SINE = (
    6.283182818832115,
    -41.34142141640176,
    81.59618421926638,
    -76.5801034177733,
    41.205405703161745,
    -12.271277356143528,
)


def sine_of_turns(r):
    square = r * r
    value = SINE[-1] * square + SINE[-2]
    for c in SINE[-3::-1]:
        value = value * square + c
    return value * r


def partial_kernel(steps, a_ref, w_ref, s_ref, out_ref, acc, change):
    step = pl.program_id(0)
    depth, width = w_ref.shape

    @pl.when(step == 0)
    def _():
        acc[...] = jnp.zeros_like(acc)

    def tile(start, size):
        def columns(offset, length):
            if isinstance(start, int):
                return pl.ds(start + offset, length)
            return pl.ds(pl.multiple_of(start + offset, LANES), length)

        for k in range(GRID):
            for g in range(depth // GROUP):
                rows = pl.ds(g * GROUP, GROUP)
                for c in range(0, size, LANES):
                    lanes = min(LANES, size - c)
                    w = w_ref[rows, columns(c, lanes)].astype(jnp.float32)
                    scaled = w * s_ref[k, rows, :lanes]
                    top = jnp.max(jnp.abs(scaled), axis=0, keepdims=True)
                    quant_step = (top + 1e-06) / 7.0
                    v = scaled * (1.0 / quant_step)
                    wave = sine_of_turns(v - jnp.round(v))
                    wave = wave * (quant_step * (0.5 / math.pi))
                    dequant = w - wave * s_ref[GRID + k, rows, :lanes]
                    dequant = dequant.astype(jnp.bfloat16).astype(jnp.float32)
                    change[k, rows, pl.ds(c, lanes)] = (dequant - w).astype(jnp.bfloat16)
            acc[k, :, columns(0, size)] += jnp.dot(
                a_ref[...], change[k, :, pl.ds(0, size)], preferred_element_type=jnp.float32
            )

    whole = width // TILE
    if whole:

        @pl.loop(0, whole)
        def _(i):
            tile(i * TILE, TILE)

    if width % TILE:
        tile(whole * TILE, width % TILE)

    @pl.when(step == steps - 1)
    def _():
        for k in range(GRID):
            out_ref[k] = acc[k].astype(out_ref.dtype)


def partial_residue(tokens, columns, table, depth, kind):
    count, channels = tokens.shape
    width = columns.shape[1]
    steps = channels // depth
    return pl.pallas_call(
        functools.partial(partial_kernel, steps),
        grid=(steps,),
        out_shape=jax.ShapeDtypeStruct((GRID, count, width), kind),
        in_specs=[
            pl.BlockSpec((count, depth), lambda i: (0, i)),
            pl.BlockSpec((depth, width), lambda i: (i, 0)),
            pl.BlockSpec((2 * GRID, depth, LANES), lambda i: (0, i, 0)),
        ],
        out_specs=pl.BlockSpec((GRID, count, width), lambda i: (0, 0, 0)),
        scratch_shapes=[
            pltpu.VMEM((GRID, count, width), jnp.float32),
            pltpu.VMEM((GRID, depth, min(TILE, -(-width // LANES) * LANES)), jnp.bfloat16),
        ],
        compiler_params=pltpu.CompilerParams(
            dimension_semantics=("arbitrary",), vmem_limit_bytes=48 << 20
        ),
        cost_estimate=pl.CostEstimate(
            flops=30 * GRID * channels * width * 16,
            bytes_accessed=4 * channels * width,
            transcendentals=0,
        ),
    )(tokens, columns, table)


def in_halves(activations, weight):
    n = lax.axis_size("dp")
    half = n // 2
    me = lax.axis_index("dp")
    side, place = me // half, me % half
    groups = [list(range(half)), list(range(half, n))]
    across = [(i, (i + half) % n) for i in range(n)]

    widened = lax.all_gather(activations, "tensor", axis=1, tiled=True)
    own_tokens, channels = widened.shape
    mine = channels // 2
    token_count = own_tokens * n
    kept = lax.dynamic_slice_in_dim(widened, side * mine, mine, axis=1)
    away = lax.dynamic_slice_in_dim(widened, (1 - side) * mine, mine, axis=1)
    other = lax.ppermute(away, "dp", across)
    first = side == 0
    pair = jnp.concatenate([jnp.where(first, kept, other), jnp.where(first, other, kept)], axis=0)
    tokens = lax.all_gather(pair, "dp", axis=0, tiled=True, axis_index_groups=groups)

    width = weight.shape[1]
    away_weight = lax.dynamic_slice_in_dim(weight, (1 - side) * (width // 2), width // 2, axis=1)
    kept_weight = lax.dynamic_slice_in_dim(weight, side * (width // 2), width // 2, axis=1)
    exchange = functools.partial(
        lax.all_to_all, axis_name="dp", split_axis=1, concat_axis=0, tiled=True, axis_index_groups=groups
    )
    away_columns = exchange(away_weight)
    kept_columns = exchange(kept_weight)

    half_mean = jnp.sum(jnp.abs(tokens.astype(jnp.float32)), axis=0) / token_count + 1e-06
    other_mean = lax.ppermute(half_mean, "dp", across)
    ratios = jnp.arange(GRID, dtype=jnp.float32) / GRID
    raw = jnp.exp(ratios[:, None] * jnp.log(half_mean)[None, :])
    raw_other = jnp.exp(ratios[:, None] * jnp.log(other_mean)[None, :])
    top = jnp.maximum(jnp.max(raw, axis=1, keepdims=True), jnp.max(raw_other, axis=1, keepdims=True))
    bottom = jnp.minimum(jnp.min(raw, axis=1, keepdims=True), jnp.min(raw_other, axis=1, keepdims=True))
    scales = raw / jnp.sqrt(top * bottom)
    table = jnp.concatenate([scales, 1.0 / scales], axis=0)
    table = jnp.broadcast_to(table[:, :, None], (2 * GRID, mine, LANES))

    depth = weight.shape[0]
    away_part = partial_residue(tokens, away_columns, table, depth, jnp.bfloat16)
    arrived = lax.ppermute(away_part, "dp", across)
    own_part = partial_residue(tokens, kept_columns, table, depth, jnp.float32)
    residue = own_part + arrived.astype(jnp.float32)
    column_sums = jnp.sum(residue * residue, axis=1)

    totals = lax.psum(jnp.sum(column_sums, axis=1), ("dp", "tensor"))
    errors = totals / (token_count * width * lax.axis_size("tensor"))
    column_errors = column_sums / token_count
    own_mean = lax.dynamic_slice_in_dim(half_mean, place * depth, depth)
    return (own_mean, column_errors, errors)


PLANES = 4
CHUNK = LANES
BLOCK = 512
AHEAD = 4
SKEW = 2
BOW = (12.568868617017895, 50.02489230906822, 77.93933755195671)
BOW_SHIFT = BOW[1] / (2.0 * BOW[2])
BOW_FLOOR = BOW[0] / BOW[2] - BOW_SHIFT * BOW_SHIFT


def change_of(w16, scale, unscale):
    w = w16.astype(jnp.float32)
    scaled = w if scale is None else w * scale
    top = jnp.max(jnp.abs(scaled), axis=0, keepdims=True) + 1e-06
    v = scaled * (7.0 / top)
    r = v - jnp.round(v)
    size = jnp.abs(r)
    rest = 0.5 - size
    m = size * rest + BOW_SHIFT
    wave = (r * rest) * (m * m + BOW_FLOOR) * (top * (BOW[2] / (14.0 * math.pi)))
    if unscale is not None:
        wave = wave * unscale
    return (w - wave).astype(jnp.bfloat16) - w16


def fused_kernel(
    n, a_ref, w_ref, mean_ref, col_ref, err_ref,
    wbuf, abuf, astage, table, meanrow, change, acc, stage, recv, colsum, cbuf, mine, theirs, etile, etiles, ztile, ztiles,
    w_send, w_recv, az_send, az_recv, ab_send, ab_recv, mm_send, mm_recv, p_send, p_recv, c_send, c_recv, e_send, e_recv, t_send, t_recv,
):
    depth = w_ref.shape[0]
    plane = n // PLANES
    channels = plane * depth
    chunks = wbuf.shape[0]
    half, per = chunks // 2, chunks // PLANES
    tokens = abuf.shape[0]
    own = tokens // n
    rows_each = own * PLANES
    me = lax.axis_index("dp")
    z, p = me // plane, me % plane
    partner = p + 1 - 2 * (p % 2)

    def copy_to(device, source, target, send, arrive):
        return pltpu.make_async_remote_copy(
            src_ref=source, dst_ref=target, send_sem=send, recv_sem=arrive,
            device_id={"dp": device}, device_id_type=pl.DeviceIdType.MESH,
        )

    def settle(ref, sem):
        pltpu.make_async_copy(ref, ref, sem).wait()

    barrier = pltpu.get_barrier_semaphore()

    near = [z * plane + (p + j) % plane for j in range(1, plane)]
    near += [(z + i) % PLANES * plane + p for i in range(1, PLANES)]
    for device in near:
        pl.semaphore_signal(barrier, inc=1, device_id={"dp": device}, device_id_type=pl.DeviceIdType.MESH)
    pl.semaphore_wait(barrier, len(near))

    def slab(at):
        return a_ref.at[:, pl.ds(pl.multiple_of(at * channels, channels), channels)]

    def z_copy(i):
        to = (z + i) % PLANES
        return copy_to(to * plane + p, slab(to), astage.at[z], az_send.at[i], az_recv.at[z])

    for i in range(1, PLANES):
        z_copy(i).start()
    pltpu.make_async_copy(slab(z), astage.at[z], az_recv.at[z]).start()

    lead = jnp.where(z < PLANES // 2, 1, 0)
    skew = jnp.where((z == 0) | (z == PLANES - 1), SKEW, 0)

    def chunk_of(step):
        early = step <= skew
        late = step >= chunks - 1 - skew
        even = (step + skew) % 2 == 0
        side = jnp.where(early | (even & jnp.logical_not(late)), lead, 1 - lead)
        middle = jnp.where(even, (step + skew) // 2, (step + chunks - skew - 1) // 2 - half)
        return side * half + jnp.where(early, step, jnp.where(late, step - half, middle))

    def send_weights(step):
        c = chunk_of(step)
        rows = pl.ds(pl.multiple_of(p * depth, depth), depth)

        def piece(q):
            at = pl.multiple_of(((c // per) * plane * per + q * per + c % per) * CHUNK, CHUNK)
            return w_ref.at[:, pl.ds(at, CHUNK)]

        @pl.loop(1, plane)
        def _(j):
            q = (p + j) % plane
            copy_to(z * plane + q, piece(q), wbuf.at[c, rows, :], w_send.at[c], w_recv.at[c]).start()

        pltpu.make_async_copy(piece(p), wbuf.at[c, rows, :], w_recv.at[c]).start()

    send_weights(0)

    for i in range(PLANES):
        settle(astage.at[i], az_recv.at[i])

    def block(q):
        return abuf.at[pl.ds(pl.multiple_of(q * rows_each, rows_each), rows_each), :]

    @pl.loop(0, channels // LANES)
    def _(i):
        lanes = pl.ds(pl.multiple_of(i * LANES, LANES), LANES)
        part = [astage[t, :, lanes].astype(jnp.float32) for t in range(PLANES)]
        whole = jnp.concatenate(part, axis=0).astype(jnp.bfloat16)
        abuf[pl.ds(pl.multiple_of(p * rows_each, rows_each), rows_each), lanes] = whole

    for j in range(1, plane // 2):
        to = (p + 2 * j) % plane
        copy_to(z * plane + to, block(p), block(p), ab_send.at[j], ab_recv.at[p]).start()
    copy_to(z * plane + partner, block(p), block(p), ab_send.at[0], ab_recv.at[p]).start()

    for step in range(1, AHEAD):
        send_weights(step)

    for j in range(1, plane // 2):
        q = (p + 2 * j) % plane
        settle(block(q), ab_recv.at[q])
        copy_to(z * plane + partner, block(q), block(q), ab_send.at[plane // 2 + j - 1], ab_recv.at[q]).start()
    for j in range(plane // 2):
        q = (partner + 2 * j) % plane
        settle(block(q), ab_recv.at[q])

    def means(i, carry):
        most, least = carry
        lanes = pl.ds(pl.multiple_of(i * LANES, LANES), LANES)
        sums = jnp.sum(jnp.abs(abuf[:, lanes].astype(jnp.float32)), axis=0, keepdims=True)
        mean = sums / tokens + 1e-06
        meanrow[:, lanes] = mean
        table[0, lanes, :] = jnp.transpose(jnp.broadcast_to(jnp.log(mean), (LANES, LANES)))
        return jnp.maximum(most, mean), jnp.minimum(least, mean)

    most, least = lax.fori_loop(
        0, channels // LANES, means,
        (jnp.zeros((1, LANES), jnp.float32), jnp.full((1, LANES), jnp.inf, jnp.float32)),
    )
    mean_ref[...] = meanrow[:, pl.ds(pl.multiple_of(p * depth, depth), depth)]
    mine[0:1, :] = most
    mine[1:2, :] = least

    def mm_copy(i):
        to = (z + i) % PLANES
        return copy_to(to * plane + p, mine, theirs.at[i], mm_send.at[i], mm_recv.at[i])

    for i in range(1, PLANES):
        mm_copy(i).start()
    for i in range(1, PLANES):
        settle(theirs.at[i], mm_recv.at[i])
        most = jnp.maximum(most, theirs[i, 0:1, :])
        least = jnp.minimum(least, theirs[i, 1:2, :])
    ends = jnp.log(jnp.max(most, axis=1, keepdims=True)) + jnp.log(jnp.min(least, axis=1, keepdims=True))
    middle = 0.5 * ends

    @pl.loop(0, channels // LANES)
    def _(i):
        rows = pl.ds(pl.multiple_of(i * LANES, LANES), LANES)
        level = table[0, rows, :] - middle
        for k in range(1, GRID):
            table[2 * k - 2, rows, :] = jnp.exp((k / GRID) * level)
            table[2 * k - 1, rows, :] = jnp.exp((-k / GRID) * level)

    def add_product(pair, base):
        lhs = abuf[:, pl.ds(base, BLOCK)]
        acc[pair] += jnp.dot(lhs, change[pair], preferred_element_type=jnp.float32)

    def partial_products(c):
        acc[...] = jnp.zeros_like(acc)
        change[1] = jnp.zeros_like(change[1])

        @pl.loop(0, channels // BLOCK)
        def _(b):
            base = pl.multiple_of(b * BLOCK, BLOCK)
            add_product(1, pl.multiple_of(jnp.maximum(base - BLOCK, 0), BLOCK))
            for pair in range(GRID // 2):
                for k in (2 * pair, 2 * pair + 1):
                    for g in range(BLOCK // GROUP):
                        rows = pl.ds(base + g * GROUP, GROUP)
                        scale = table[2 * k - 2, rows, :] if k else None
                        unscale = table[2 * k - 1, rows, :] if k else None
                        change[pair, pl.ds(g * GROUP, GROUP), pl.ds(k % 2 * CHUNK, CHUNK)] = change_of(
                            wbuf[c, rows, :], scale, unscale
                        )
                if pair == 0:
                    add_product(0, base)

        add_product(1, channels - BLOCK)

    def hand_on(c, k, to):
        return copy_to(to * plane + p, stage.at[c, k], recv.at[c, k], p_send.at[c, k], p_recv.at[c, k])

    steps = chunks
    for_side = ((PLANES - 1 - z, z - 1), (z, z + 1))

    @pl.loop(0, steps - 1 + 2 * (PLANES - 2))
    def _(step):
        @pl.when(step < steps)
        def _():
            c = chunk_of(step)

            @pl.when(step + AHEAD < steps)
            def _():
                send_weights(step + AHEAD)

            settle(wbuf.at[c], w_recv.at[c])
            partial_products(c)
            for k in range(GRID):
                stage[c, k] = acc[k // 2, :, k % 2 * CHUNK : (k % 2 + 1) * CHUNK].astype(jnp.bfloat16)
            for side in range(2):
                gone, to = for_side[side]

                @pl.when((c // half == side) & (gone == 0))
                def _():
                    for k in range(GRID):
                        hand_on(c, k, to).start()

        for side in range(2):
            gone, to = for_side[side]
            turn = step - 2 * (gone - 1)
            index = jnp.where(turn < 2 * SKEW, turn - SKEW, turn // 2)
            c = side * half + index
            due = (turn % 2 == 0) | (turn < 2 * SKEW)
            ready = (gone > 0) & (turn >= SKEW) & due & (index < half)

            @pl.when(ready & (gone < PLANES - 1))
            def _():
                for k in range(GRID):
                    settle(recv.at[c, k], p_recv.at[c, k])
                    total = stage[c, k].astype(jnp.float32) + recv[c, k].astype(jnp.float32)
                    stage[c, k] = total.astype(jnp.bfloat16)
                    hand_on(c, k, to).start()

            @pl.when(ready & (gone == PLANES - 1))
            def _():
                for k in range(GRID):
                    settle(recv.at[c, k], p_recv.at[c, k])
                    residue = stage[c, k].astype(jnp.float32) + recv[c, k].astype(jnp.float32)
                    sums = jnp.sum(residue * residue, axis=0, keepdims=True)
                    for h in range(0, CHUNK, LANES):
                        at = c * CHUNK + h
                        width = colsum.shape[2]
                        lanes = pl.ds(pl.multiple_of(at % width, LANES), LANES)
                        colsum[at // width, k : k + 1, lanes] = sums[:, h : h + LANES]

    finishing = (z == 0) | (z == PLANES - 1)
    first_block = jnp.where(z == 0, 0, PLANES // 2)
    end = jnp.where(z == 0, 0, 1)

    def column_copy(i):
        j = first_block + i
        return copy_to(j * plane + p, colsum.at[j], cbuf, c_send.at[i], c_recv)

    def total_copy(j):
        return copy_to(z * plane + (p + j) % plane, etile, etiles.at[p], e_send.at[j], e_recv.at[p])

    def line_copy(i):
        return copy_to((z + i) % PLANES * plane + p, ztile, ztiles.at[end], t_send.at[i], t_recv.at[end])

    @pl.when(finishing)
    def _():
        for i in range(PLANES // 2):
            to_self = first_block + i == z

            @pl.when(jnp.logical_not(to_self))
            def _():
                column_copy(i).start()

            @pl.when(to_self)
            def _():
                cbuf[...] = colsum[first_block + i]

        total = jnp.zeros((8, 1), jnp.float32)
        for i in range(PLANES // 2):
            total += jnp.sum(colsum[first_block + i], axis=1, keepdims=True)
        etile[...] = jnp.broadcast_to(total, (8, LANES))
        for j in range(1, plane):
            total_copy(j).start()
        etiles[p] = etile[...]
        for j in range(1, plane):
            q = (p + j) % plane
            settle(etiles.at[q], e_recv.at[q])
        total = etiles[0]
        for q in range(1, plane):
            total += etiles[q]
        ztile[...] = total
        for i in range(1, PLANES):
            line_copy(i).start()
        ztiles[end] = total

    @pl.when(jnp.logical_not(finishing))
    def _():
        settle(cbuf, c_recv)

    col_ref[...] = cbuf[...] * (1.0 / tokens)
    for i in range(2):

        @pl.when(z != i * (PLANES - 1))
        def _():
            settle(ztiles.at[i], t_recv.at[i])

    err_ref[...] = (ztiles[0] + ztiles[1]) * (1.0 / (tokens * plane * chunks * CHUNK))

    for i in range(1, PLANES):
        z_copy(i).wait_send()
        mm_copy(i).wait_send()
    for i in range(plane - 1):
        settle(block(0), ab_send.at[i])

    @pl.loop(0, chunks)
    def _(c):
        settle(wbuf.at[0, pl.ds(0, channels - depth), :], w_send.at[c])

        for side in range(2):
            gone, to = for_side[side]

            @pl.when((c // half == side) & (gone < PLANES - 1))
            def _():
                for k in range(GRID):
                    settle(stage.at[c, k], p_send.at[c, k])

    @pl.when(finishing)
    def _():
        for i in range(PLANES // 2):

            @pl.when(first_block + i != z)
            def _():
                settle(colsum.at[0], c_send.at[i])

        for j in range(1, plane):
            settle(etile, e_send.at[j])
        for i in range(1, PLANES):
            settle(ztile, t_send.at[i])


def in_one_kernel(activations, weight):
    n = lax.axis_size("dp")
    own, depth = activations.shape[0], weight.shape[0]
    plane = n // PLANES
    channels, tokens = plane * depth, n * own
    chunks = weight.shape[1] // (plane * CHUNK)
    width = weight.shape[1] // n
    dma, f32, bf16 = pltpu.SemaphoreType.DMA, jnp.float32, jnp.bfloat16
    mean, columns, errors = pl.pallas_call(
        functools.partial(fused_kernel, n),
        out_shape=(
            jax.ShapeDtypeStruct((1, depth), f32),
            jax.ShapeDtypeStruct((8, width), f32),
            jax.ShapeDtypeStruct((8, LANES), f32),
        ),
        in_specs=[pl.BlockSpec(memory_space=pl.ANY)] * 2,
        out_specs=[pl.BlockSpec(memory_space=pltpu.VMEM)] * 3,
        scratch_shapes=[
            pltpu.VMEM((chunks, channels, CHUNK), bf16),
            pltpu.VMEM((tokens, channels), bf16),
            pltpu.VMEM((PLANES, own, channels), bf16),
            pltpu.VMEM((2 * GRID - 2, channels, LANES), f32),
            pltpu.VMEM((1, channels), f32),
            pltpu.VMEM((GRID // 2, BLOCK, 2 * CHUNK), bf16),
            pltpu.VMEM((GRID // 2, tokens, 2 * CHUNK), f32),
            pltpu.VMEM((chunks, GRID, tokens, CHUNK), bf16),
            pltpu.VMEM((chunks, GRID, tokens, CHUNK), bf16),
            pltpu.VMEM((PLANES, 8, width), f32),
            pltpu.VMEM((8, width), f32),
            pltpu.VMEM((8, LANES), f32),
            pltpu.VMEM((PLANES, 8, LANES), f32),
            pltpu.VMEM((8, LANES), f32),
            pltpu.VMEM((plane, 8, LANES), f32),
            pltpu.VMEM((8, LANES), f32),
            pltpu.VMEM((2, 8, LANES), f32),
            dma((chunks,)), dma((chunks,)),
            dma((PLANES,)), dma((PLANES,)),
            dma((plane,)), dma((plane,)),
            dma((PLANES,)), dma((PLANES,)),
            dma((chunks, GRID)), dma((chunks, GRID)),
            dma((PLANES // 2,)), dma,
            dma((plane,)), dma((plane,)),
            dma((PLANES,)), dma((2,)),
        ],
        compiler_params=pltpu.CompilerParams(
            collective_id=0, has_side_effects=True, vmem_limit_bytes=62 << 20
        ),
    )(activations, weight)
    return (mean.reshape(depth), columns[:GRID], errors[:GRID, 0])


def one_kernel_fits(activations, weight):
    n, tensor = lax.axis_size("dp"), lax.axis_size("tensor")
    if tensor != 1 or n % (2 * PLANES) or n < 4 * PLANES:
        return False
    plane = n // PLANES
    channels, width = plane * weight.shape[0], weight.shape[1]
    aligned = (activations.shape[0] * PLANES) % 16 == 0 and weight.shape[0] % GROUP == 0
    return aligned and channels % BLOCK == 0 and width % (CHUNK * n) == 0


def on_device(activations, weight):
    if one_kernel_fits(activations, weight):
        return in_one_kernel(activations, weight)
    return in_halves(activations, weight)


def solution(mesh):
    placed = (P("dp", "tensor"), P("dp", "tensor"))
    return jax.shard_map(
        on_device,
        mesh=mesh,
        in_specs=placed,
        out_specs=(P("dp"), P(None, ("tensor", "dp")), P()),
        check_vma=False,
    )
```

```python
import functools
import math

import jax
import jax.numpy as jnp
from jax import lax
from jax.experimental import pallas as pl
from jax.experimental.pallas import tpu as pltpu
from jax.sharding import PartitionSpec as P

GROUP = 128
GRID = 4
LANES = 128
TILE = 256
SINE = (
    6.283182818832115,
    -41.34142141640176,
    81.59618421926638,
    -76.5801034177733,
    41.205405703161745,
    -12.271277356143528,
)


def sine_of_turns(r):
    square = r * r
    value = SINE[-1] * square + SINE[-2]
    for c in SINE[-3::-1]:
        value = value * square + c
    return value * r


def partial_kernel(steps, a_ref, w_ref, s_ref, out_ref, acc, change):
    step = pl.program_id(0)
    depth, width = w_ref.shape

    @pl.when(step == 0)
    def _():
        acc[...] = jnp.zeros_like(acc)

    def tile(start, size):
        def columns(offset, length):
            if isinstance(start, int):
                return pl.ds(start + offset, length)
            return pl.ds(pl.multiple_of(start + offset, LANES), length)

        for k in range(GRID):
            for g in range(depth // GROUP):
                rows = pl.ds(g * GROUP, GROUP)
                for c in range(0, size, LANES):
                    lanes = min(LANES, size - c)
                    w = w_ref[rows, columns(c, lanes)].astype(jnp.float32)
                    scaled = w * s_ref[k, rows, :lanes]
                    top = jnp.max(jnp.abs(scaled), axis=0, keepdims=True)
                    quant_step = (top + 1e-06) / 7.0
                    v = scaled * (1.0 / quant_step)
                    wave = sine_of_turns(v - jnp.round(v))
                    wave = wave * (quant_step * (0.5 / math.pi))
                    dequant = w - wave * s_ref[GRID + k, rows, :lanes]
                    dequant = dequant.astype(jnp.bfloat16).astype(jnp.float32)
                    change[k, rows, pl.ds(c, lanes)] = (dequant - w).astype(jnp.bfloat16)
            acc[k, :, columns(0, size)] += jnp.dot(
                a_ref[...], change[k, :, pl.ds(0, size)], preferred_element_type=jnp.float32
            )

    whole = width // TILE
    if whole:

        @pl.loop(0, whole)
        def _(i):
            tile(i * TILE, TILE)

    if width % TILE:
        tile(whole * TILE, width % TILE)

    @pl.when(step == steps - 1)
    def _():
        for k in range(GRID):
            out_ref[k] = acc[k].astype(out_ref.dtype)


def partial_residue(tokens, columns, table, depth, kind):
    count, channels = tokens.shape
    width = columns.shape[1]
    steps = channels // depth
    return pl.pallas_call(
        functools.partial(partial_kernel, steps),
        grid=(steps,),
        out_shape=jax.ShapeDtypeStruct((GRID, count, width), kind),
        in_specs=[
            pl.BlockSpec((count, depth), lambda i: (0, i)),
            pl.BlockSpec((depth, width), lambda i: (i, 0)),
            pl.BlockSpec((2 * GRID, depth, LANES), lambda i: (0, i, 0)),
        ],
        out_specs=pl.BlockSpec((GRID, count, width), lambda i: (0, 0, 0)),
        scratch_shapes=[
            pltpu.VMEM((GRID, count, width), jnp.float32),
            pltpu.VMEM((GRID, depth, min(TILE, -(-width // LANES) * LANES)), jnp.bfloat16),
        ],
        compiler_params=pltpu.CompilerParams(
            dimension_semantics=("arbitrary",), vmem_limit_bytes=48 << 20
        ),
        cost_estimate=pl.CostEstimate(
            flops=30 * GRID * channels * width * 16,
            bytes_accessed=4 * channels * width,
            transcendentals=0,
        ),
    )(tokens, columns, table)


def in_halves(activations, weight):
    n = lax.axis_size("dp")
    half = n // 2
    me = lax.axis_index("dp")
    side, place = me // half, me % half
    groups = [list(range(half)), list(range(half, n))]
    across = [(i, (i + half) % n) for i in range(n)]

    widened = lax.all_gather(activations, "tensor", axis=1, tiled=True)
    own_tokens, channels = widened.shape
    mine = channels // 2
    token_count = own_tokens * n
    kept = lax.dynamic_slice_in_dim(widened, side * mine, mine, axis=1)
    away = lax.dynamic_slice_in_dim(widened, (1 - side) * mine, mine, axis=1)
    other = lax.ppermute(away, "dp", across)
    first = side == 0
    pair = jnp.concatenate([jnp.where(first, kept, other), jnp.where(first, other, kept)], axis=0)
    tokens = lax.all_gather(pair, "dp", axis=0, tiled=True, axis_index_groups=groups)

    width = weight.shape[1]
    away_weight = lax.dynamic_slice_in_dim(weight, (1 - side) * (width // 2), width // 2, axis=1)
    kept_weight = lax.dynamic_slice_in_dim(weight, side * (width // 2), width // 2, axis=1)
    exchange = functools.partial(
        lax.all_to_all, axis_name="dp", split_axis=1, concat_axis=0, tiled=True, axis_index_groups=groups
    )
    away_columns = exchange(away_weight)
    kept_columns = exchange(kept_weight)

    half_mean = jnp.sum(jnp.abs(tokens.astype(jnp.float32)), axis=0) / token_count + 1e-06
    other_mean = lax.ppermute(half_mean, "dp", across)
    ratios = jnp.arange(GRID, dtype=jnp.float32) / GRID
    raw = jnp.exp(ratios[:, None] * jnp.log(half_mean)[None, :])
    raw_other = jnp.exp(ratios[:, None] * jnp.log(other_mean)[None, :])
    top = jnp.maximum(jnp.max(raw, axis=1, keepdims=True), jnp.max(raw_other, axis=1, keepdims=True))
    bottom = jnp.minimum(jnp.min(raw, axis=1, keepdims=True), jnp.min(raw_other, axis=1, keepdims=True))
    scales = raw / jnp.sqrt(top * bottom)
    table = jnp.concatenate([scales, 1.0 / scales], axis=0)
    table = jnp.broadcast_to(table[:, :, None], (2 * GRID, mine, LANES))

    depth = weight.shape[0]
    away_part = partial_residue(tokens, away_columns, table, depth, jnp.bfloat16)
    arrived = lax.ppermute(away_part, "dp", across)
    own_part = partial_residue(tokens, kept_columns, table, depth, jnp.float32)
    residue = own_part + arrived.astype(jnp.float32)
    column_sums = jnp.sum(residue * residue, axis=1)

    totals = lax.psum(jnp.sum(column_sums, axis=1), ("dp", "tensor"))
    errors = totals / (token_count * width * lax.axis_size("tensor"))
    column_errors = column_sums / token_count
    own_mean = lax.dynamic_slice_in_dim(half_mean, place * depth, depth)
    return (own_mean, column_errors, errors)


PLANES = 4
CHUNK = LANES
BLOCK = 512
AHEAD = 4
SKEW = 2
EARLY = 4
BOW = (12.568868617017895, 50.02489230906822, 77.93933755195671)
BOW_SHIFT = BOW[1] / (2.0 * BOW[2])
BOW_FLOOR = BOW[0] / BOW[2] - BOW_SHIFT * BOW_SHIFT


def change_of(w16, scale, unscale):
    w = w16.astype(jnp.float32)
    scaled = w if scale is None else w * scale
    top = jnp.max(jnp.abs(scaled), axis=0, keepdims=True) + 1e-06
    v = scaled * (7.0 / top)
    r = v - jnp.round(v)
    size = jnp.abs(r)
    rest = 0.5 - size
    m = size * rest + BOW_SHIFT
    wave = (r * rest) * (m * m + BOW_FLOOR) * (top * (BOW[2] / (14.0 * math.pi)))
    if unscale is not None:
        wave = wave * unscale
    return (w - wave).astype(jnp.bfloat16) - w16


def fused_kernel(
    n, a_ref, w_ref, mean_ref, col_ref, err_ref,
    wbuf, abuf, astage, table, meanrow, change, acc, stage, recv, colsum, cbuf, mine, theirs, etile, etiles, ztile, ztiles, inward,
    w_send, w_recv, az_send, az_recv, ab_send, ab_recv, mm_send, mm_recv, p_send, p_recv, c_send, c_recv, e_send, e_recv, t_send, t_recv, i_send, i_recv,
):
    depth = w_ref.shape[0]
    plane = n // PLANES
    channels = plane * depth
    chunks = wbuf.shape[0]
    half, per = chunks // 2, chunks // PLANES
    tokens = abuf.shape[0]
    own = tokens // n
    rows_each = own * PLANES
    me = lax.axis_index("dp")
    z, p = me // plane, me % plane
    partner = p + 1 - 2 * (p % 2)

    def copy_to(device, source, target, send, arrive):
        return pltpu.make_async_remote_copy(
            src_ref=source, dst_ref=target, send_sem=send, recv_sem=arrive,
            device_id={"dp": device}, device_id_type=pl.DeviceIdType.MESH,
        )

    def settle(ref, sem):
        pltpu.make_async_copy(ref, ref, sem).wait()

    barrier = pltpu.get_barrier_semaphore()

    near = [z * plane + (p + j) % plane for j in range(1, plane)]
    near += [(z + i) % PLANES * plane + p for i in range(1, PLANES)]
    for device in near:
        pl.semaphore_signal(barrier, inc=1, device_id={"dp": device}, device_id_type=pl.DeviceIdType.MESH)
    pl.semaphore_wait(barrier, len(near))

    def slab(at):
        return a_ref.at[:, pl.ds(pl.multiple_of(at * channels, channels), channels)]

    def z_copy(i):
        to = (z + i) % PLANES
        return copy_to(to * plane + p, slab(to), astage.at[z], az_send.at[i], az_recv.at[z])

    for i in range(1, PLANES):
        z_copy(i).start()
    pltpu.make_async_copy(slab(z), astage.at[z], az_recv.at[z]).start()

    lead = jnp.where(z < PLANES // 2, 1, 0)
    skew = jnp.where((z == 0) | (z == PLANES - 1), SKEW, 0)

    def place_of(side, index):
        return jnp.where(side == 0, index, chunks - 1 - index)

    def chunk_of(step):
        early = step <= skew
        late = step >= chunks - 1 - skew
        even = (step + skew) % 2 == 0
        side = jnp.where(early | (even & jnp.logical_not(late)), lead, 1 - lead)
        middle = jnp.where(even, (step + skew) // 2, (step + chunks - skew - 1) // 2 - half)
        index = jnp.where(early, step, jnp.where(late, step - half, middle))
        moved = (skew > 0) & (side != lead) & (index >= half - EARLY)
        index = jnp.where(moved, jnp.where(index == half - EARLY, half - 1, index - 1), index)
        return place_of(side, index)

    def send_weights(step):
        c = chunk_of(step)
        rows = pl.ds(pl.multiple_of(p * depth, depth), depth)

        def piece(q):
            at = pl.multiple_of(((c // per) * plane * per + q * per + c % per) * CHUNK, CHUNK)
            return w_ref.at[:, pl.ds(at, CHUNK)]

        @pl.loop(1, plane)
        def _(j):
            q = (p + j) % plane
            copy_to(z * plane + q, piece(q), wbuf.at[c, rows, :], w_send.at[c], w_recv.at[c]).start()

        pltpu.make_async_copy(piece(p), wbuf.at[c, rows, :], w_recv.at[c]).start()

    send_weights(0)

    for i in range(PLANES):
        settle(astage.at[i], az_recv.at[i])

    def block(q):
        return abuf.at[pl.ds(pl.multiple_of(q * rows_each, rows_each), rows_each), :]

    @pl.loop(0, channels // LANES)
    def _(i):
        lanes = pl.ds(pl.multiple_of(i * LANES, LANES), LANES)
        part = [astage[t, :, lanes].astype(jnp.float32) for t in range(PLANES)]
        whole = jnp.concatenate(part, axis=0).astype(jnp.bfloat16)
        abuf[pl.ds(pl.multiple_of(p * rows_each, rows_each), rows_each), lanes] = whole

    for j in range(1, plane // 2):
        to = (p + 2 * j) % plane
        copy_to(z * plane + to, block(p), block(p), ab_send.at[j], ab_recv.at[p]).start()
    copy_to(z * plane + partner, block(p), block(p), ab_send.at[0], ab_recv.at[p]).start()

    for step in range(1, AHEAD):
        send_weights(step)

    for j in range(1, plane // 2):
        q = (p + 2 * j) % plane
        settle(block(q), ab_recv.at[q])
        copy_to(z * plane + partner, block(q), block(q), ab_send.at[plane // 2 + j - 1], ab_recv.at[q]).start()
    for j in range(plane // 2):
        q = (partner + 2 * j) % plane
        settle(block(q), ab_recv.at[q])

    def means(i, carry):
        most, least = carry
        lanes = pl.ds(pl.multiple_of(i * LANES, LANES), LANES)
        sums = jnp.sum(jnp.abs(abuf[:, lanes].astype(jnp.float32)), axis=0, keepdims=True)
        mean = sums / tokens + 1e-06
        meanrow[:, lanes] = mean
        table[0, lanes, :] = jnp.transpose(jnp.broadcast_to(jnp.log(mean), (LANES, LANES)))
        return jnp.maximum(most, mean), jnp.minimum(least, mean)

    most, least = lax.fori_loop(
        0, channels // LANES, means,
        (jnp.zeros((1, LANES), jnp.float32), jnp.full((1, LANES), jnp.inf, jnp.float32)),
    )
    mean_ref[...] = meanrow[:, pl.ds(pl.multiple_of(p * depth, depth), depth)]
    mine[0:1, :] = most
    mine[1:2, :] = least

    def mm_copy(i):
        to = (z + i) % PLANES
        return copy_to(to * plane + p, mine, theirs.at[i], mm_send.at[i], mm_recv.at[i])

    for i in range(1, PLANES):
        mm_copy(i).start()
    for i in range(1, PLANES):
        settle(theirs.at[i], mm_recv.at[i])
        most = jnp.maximum(most, theirs[i, 0:1, :])
        least = jnp.minimum(least, theirs[i, 1:2, :])
    ends = jnp.log(jnp.max(most, axis=1, keepdims=True)) + jnp.log(jnp.min(least, axis=1, keepdims=True))
    middle = 0.5 * ends

    @pl.loop(0, channels // LANES)
    def _(i):
        rows = pl.ds(pl.multiple_of(i * LANES, LANES), LANES)
        level = table[0, rows, :] - middle
        for k in range(1, GRID):
            table[2 * k - 2, rows, :] = jnp.exp((k / GRID) * level)
            table[2 * k - 1, rows, :] = jnp.exp((-k / GRID) * level)

    def add_product(pair, base):
        lhs = abuf[:, pl.ds(base, BLOCK)]
        acc[pair] += jnp.dot(lhs, change[pair], preferred_element_type=jnp.float32)

    def partial_products(c):
        acc[...] = jnp.zeros_like(acc)
        change[1] = jnp.zeros_like(change[1])

        @pl.loop(0, channels // BLOCK)
        def _(b):
            base = pl.multiple_of(b * BLOCK, BLOCK)
            add_product(1, pl.multiple_of(jnp.maximum(base - BLOCK, 0), BLOCK))
            for pair in range(GRID // 2):
                for k in (2 * pair, 2 * pair + 1):
                    for g in range(BLOCK // GROUP):
                        rows = pl.ds(base + g * GROUP, GROUP)
                        scale = table[2 * k - 2, rows, :] if k else None
                        unscale = table[2 * k - 1, rows, :] if k else None
                        change[pair, pl.ds(g * GROUP, GROUP), pl.ds(k % 2 * CHUNK, CHUNK)] = change_of(
                            wbuf[c, rows, :], scale, unscale
                        )
                if pair == 0:
                    add_product(0, base)

        add_product(1, channels - BLOCK)

    def hand_inward(c, k, to):
        return copy_to(to * plane + p, stage.at[c, k], inward.at[k], i_send.at[k], i_recv.at[k])

    def hand_on(c, k, to):
        return copy_to(to * plane + p, stage.at[c, k], recv.at[c, k], p_send.at[c, k], p_recv.at[c, k])

    steps = chunks
    for_side = ((PLANES - 1 - z, z - 1), (z, z + 1))
    last_of = (half - 1, half)

    colsum[...] = jnp.zeros_like(colsum)

    @pl.loop(0, steps - 1 + 2 * (PLANES - 2))
    def _(step):
        @pl.when(step < steps)
        def _():
            c = chunk_of(step)

            @pl.when(step + AHEAD < steps)
            def _():
                send_weights(step + AHEAD)

            settle(wbuf.at[c], w_recv.at[c])
            partial_products(c)
            for k in range(GRID):
                stage[c, k] = acc[k // 2, :, k % 2 * CHUNK : (k % 2 + 1) * CHUNK].astype(jnp.bfloat16)
            for side in range(2):
                gone, to = for_side[side]

                @pl.when((c // half == side) & (gone == 0))
                def _():
                    for k in range(GRID):
                        hand_on(c, k, to).start()

                @pl.when((c == last_of[side]) & (gone == PLANES - 1))
                def _():
                    for k in range(GRID):
                        hand_inward(c, k, z + (1 - 2 * side)).start()

        for side in range(2):
            gone, to = for_side[side]
            turn = step - 2 * (gone - 1) - jnp.where(gone == PLANES - 1, 2, 0)
            index = jnp.where(turn < 2 * SKEW, turn - SKEW, turn // 2)
            c = place_of(side, index)
            inner_end = (index == half - 1) & (gone == PLANES - 2)
            due = (turn % 2 == 0) | (turn < 2 * SKEW)
            ready = (gone > 0) & (turn >= SKEW) & due & (index < half)

            @pl.when(ready & (gone < PLANES - 1) & jnp.logical_not(inner_end))
            def _():
                for k in range(GRID):
                    settle(recv.at[c, k], p_recv.at[c, k])
                    total = stage[c, k].astype(jnp.float32) + recv[c, k].astype(jnp.float32)
                    stage[c, k] = total.astype(jnp.bfloat16)
                    hand_on(c, k, to).start()

            def finish(extra):
                for k in range(GRID):
                    settle(recv.at[c, k], p_recv.at[c, k])
                    residue = stage[c, k].astype(jnp.float32) + recv[c, k].astype(jnp.float32)
                    if extra:
                        settle(inward.at[k], i_recv.at[k])
                        residue += inward[k].astype(jnp.float32)
                    sums = jnp.sum(residue * residue, axis=0, keepdims=True)
                    lanes = pl.ds(pl.multiple_of(c % per * CHUNK, CHUNK), CHUNK)
                    colsum[c // per, k : k + 1, lanes] = sums

            @pl.when(ready & (gone == PLANES - 1) & (index < half - 1))
            def _():
                finish(False)

            @pl.when(ready & inner_end)
            def _():
                finish(True)

    outer = (z == 0) | (z == PLANES - 1)
    inner = jnp.where(z == 0, 1, PLANES - 2)

    def column_copy():
        return copy_to(inner * plane + p, colsum.at[inner], cbuf, c_send, c_recv)

    def total_copy(j):
        return copy_to(z * plane + (p + j) % plane, etile, etiles.at[p], e_send.at[j], e_recv.at[p])

    def line_copy(i):
        return copy_to((z + i) % PLANES * plane + p, ztile, ztiles.at[z], t_send.at[i], t_recv.at[z])

    @pl.when(outer)
    def _():
        column_copy().start()

    total = jnp.zeros((8, 1), jnp.float32)
    for i in range(PLANES):
        total += jnp.sum(colsum[i], axis=1, keepdims=True)
    etile[...] = jnp.broadcast_to(total, (8, LANES))
    for j in range(1, plane):
        total_copy(j).start()
    etiles[p] = etile[...]
    for j in range(1, plane):
        q = (p + j) % plane
        settle(etiles.at[q], e_recv.at[q])
    total = etiles[0]
    for q in range(1, plane):
        total += etiles[q]
    ztile[...] = total
    for i in range(1, PLANES):
        line_copy(i).start()
    ztiles[z] = total

    @pl.when(outer)
    def _():
        col_ref[...] = colsum[z] * (1.0 / tokens)

    @pl.when(jnp.logical_not(outer))
    def _():
        settle(cbuf, c_recv)
        col_ref[...] = (colsum[z] + cbuf[...]) * (1.0 / tokens)

    for i in range(1, PLANES):
        settle(ztiles.at[(z + i) % PLANES], t_recv.at[(z + i) % PLANES])
    total = ztiles[0]
    for i in range(1, PLANES):
        total += ztiles[i]
    on_lane = lax.broadcasted_iota(jnp.int32, (8, LANES), 0) == lax.broadcasted_iota(jnp.int32, (8, LANES), 1)
    err_ref[...] = jnp.sum(jnp.where(on_lane, total, 0.0), axis=0, keepdims=True) * (
        1.0 / (tokens * plane * chunks * CHUNK)
    )

    for i in range(1, PLANES):
        z_copy(i).wait_send()
        mm_copy(i).wait_send()
    for i in range(plane - 1):
        settle(block(0), ab_send.at[i])

    @pl.loop(0, chunks)
    def _(c):
        settle(wbuf.at[0, pl.ds(0, channels - depth), :], w_send.at[c])

        for side in range(2):
            gone, to = for_side[side]

            passed_on = (c // half == side) & (gone < PLANES - 1)
            inner_end = (c == last_of[side]) & (gone == PLANES - 2)

            @pl.when(passed_on & jnp.logical_not(inner_end))
            def _():
                for k in range(GRID):
                    settle(stage.at[c, k], p_send.at[c, k])

    @pl.when(outer)
    def _():
        for k in range(GRID):
            settle(stage.at[0, k], i_send.at[k])
        settle(cbuf, c_send)

    for j in range(1, plane):
        settle(etile, e_send.at[j])
    for i in range(1, PLANES):
        settle(ztile, t_send.at[i])


def shape_results(mean_in, col_in, err_in, mean_ref, col_ref, err_ref):
    mean_ref[...] = mean_in[0, :]
    col_ref[...] = col_in[:GRID, :]
    err_ref[...] = err_in[0, :GRID]


def in_one_kernel(activations, weight):
    n = lax.axis_size("dp")
    own, depth = activations.shape[0], weight.shape[0]
    plane = n // PLANES
    channels, tokens = plane * depth, n * own
    chunks = weight.shape[1] // (plane * CHUNK)
    width = weight.shape[1] // n
    dma, f32, bf16 = pltpu.SemaphoreType.DMA, jnp.float32, jnp.bfloat16
    mean, columns, errors = pl.pallas_call(
        functools.partial(fused_kernel, n),
        out_shape=(
            jax.ShapeDtypeStruct((1, depth), f32),
            jax.ShapeDtypeStruct((8, width), f32),
            jax.ShapeDtypeStruct((1, LANES), f32),
        ),
        in_specs=[pl.BlockSpec(memory_space=pl.ANY)] * 2,
        out_specs=[pl.BlockSpec(memory_space=pltpu.VMEM)] * 3,
        scratch_shapes=[
            pltpu.VMEM((chunks, channels, CHUNK), bf16),
            pltpu.VMEM((tokens, channels), bf16),
            pltpu.VMEM((PLANES, own, channels), bf16),
            pltpu.VMEM((2 * GRID - 2, channels, LANES), f32),
            pltpu.VMEM((1, channels), f32),
            pltpu.VMEM((GRID // 2, BLOCK, 2 * CHUNK), bf16),
            pltpu.VMEM((GRID // 2, tokens, 2 * CHUNK), f32),
            pltpu.VMEM((chunks, GRID, tokens, CHUNK), bf16),
            pltpu.VMEM((chunks, GRID, tokens, CHUNK), bf16),
            pltpu.VMEM((PLANES, 8, width), f32),
            pltpu.VMEM((8, width), f32),
            pltpu.VMEM((8, LANES), f32),
            pltpu.VMEM((PLANES, 8, LANES), f32),
            pltpu.VMEM((8, LANES), f32),
            pltpu.VMEM((plane, 8, LANES), f32),
            pltpu.VMEM((8, LANES), f32),
            pltpu.VMEM((PLANES, 8, LANES), f32),
            pltpu.VMEM((GRID, tokens, CHUNK), bf16),
            dma((chunks,)), dma((chunks,)),
            dma((PLANES,)), dma((PLANES,)),
            dma((plane,)), dma((plane,)),
            dma((PLANES,)), dma((PLANES,)),
            dma((chunks, GRID)), dma((chunks, GRID)),
            dma, dma,
            dma((plane,)), dma((plane,)),
            dma((PLANES,)), dma((PLANES,)),
            dma((GRID,)), dma((GRID,)),
        ],
        compiler_params=pltpu.CompilerParams(
            collective_id=0, has_side_effects=True, vmem_limit_bytes=62 << 20
        ),
    )(activations, weight)
    return pl.pallas_call(
        shape_results,
        out_shape=(
            jax.ShapeDtypeStruct((depth,), f32),
            jax.ShapeDtypeStruct((GRID, width), f32),
            jax.ShapeDtypeStruct((GRID,), f32),
        ),
        in_specs=[pl.BlockSpec(memory_space=pltpu.VMEM)] * 3,
        out_specs=[pl.BlockSpec(memory_space=pltpu.VMEM)] * 3,
    )(mean, columns, errors)


def one_kernel_fits(activations, weight):
    n, tensor = lax.axis_size("dp"), lax.axis_size("tensor")
    if tensor != 1 or n % (2 * PLANES) or n < 4 * PLANES:
        return False
    plane = n // PLANES
    channels, width = plane * weight.shape[0], weight.shape[1]
    aligned = (activations.shape[0] * PLANES) % 16 == 0 and weight.shape[0] % GROUP == 0
    return aligned and channels % BLOCK == 0 and width % (CHUNK * n) == 0


def on_device(activations, weight):
    if one_kernel_fits(activations, weight):
        return in_one_kernel(activations, weight)
    return in_halves(activations, weight)


def solution(mesh):
    placed = (P("dp", "tensor"), P("dp", "tensor"))
    return jax.shard_map(
        on_device,
        mesh=mesh,
        in_specs=placed,
        out_specs=(P("dp"), P(None, ("tensor", "dp")), P()),
        check_vma=False,
    )
```

```python
import functools
import math

import jax
import jax.numpy as jnp
from jax import lax
from jax.experimental import pallas as pl
from jax.experimental.pallas import tpu as pltpu
from jax.sharding import PartitionSpec as P

GROUP = 128
GRID = 4
LANES = 128
TILE = 256
SINE = (
    6.283182818832115,
    -41.34142141640176,
    81.59618421926638,
    -76.5801034177733,
    41.205405703161745,
    -12.271277356143528,
)


def sine_of_turns(r):
    square = r * r
    value = SINE[-1] * square + SINE[-2]
    for c in SINE[-3::-1]:
        value = value * square + c
    return value * r


def partial_kernel(steps, a_ref, w_ref, s_ref, out_ref, acc, change):
    step = pl.program_id(0)
    depth, width = w_ref.shape

    @pl.when(step == 0)
    def _():
        acc[...] = jnp.zeros_like(acc)

    def tile(start, size):
        def columns(offset, length):
            if isinstance(start, int):
                return pl.ds(start + offset, length)
            return pl.ds(pl.multiple_of(start + offset, LANES), length)

        for k in range(GRID):
            for g in range(depth // GROUP):
                rows = pl.ds(g * GROUP, GROUP)
                for c in range(0, size, LANES):
                    lanes = min(LANES, size - c)
                    w = w_ref[rows, columns(c, lanes)].astype(jnp.float32)
                    scaled = w * s_ref[k, rows, :lanes]
                    top = jnp.max(jnp.abs(scaled), axis=0, keepdims=True)
                    quant_step = (top + 1e-06) / 7.0
                    v = scaled * (1.0 / quant_step)
                    wave = sine_of_turns(v - jnp.round(v))
                    wave = wave * (quant_step * (0.5 / math.pi))
                    dequant = w - wave * s_ref[GRID + k, rows, :lanes]
                    dequant = dequant.astype(jnp.bfloat16).astype(jnp.float32)
                    change[k, rows, pl.ds(c, lanes)] = (dequant - w).astype(jnp.bfloat16)
            acc[k, :, columns(0, size)] += jnp.dot(
                a_ref[...], change[k, :, pl.ds(0, size)], preferred_element_type=jnp.float32
            )

    whole = width // TILE
    if whole:

        @pl.loop(0, whole)
        def _(i):
            tile(i * TILE, TILE)

    if width % TILE:
        tile(whole * TILE, width % TILE)

    @pl.when(step == steps - 1)
    def _():
        for k in range(GRID):
            out_ref[k] = acc[k].astype(out_ref.dtype)


def partial_residue(tokens, columns, table, depth, kind):
    count, channels = tokens.shape
    width = columns.shape[1]
    steps = channels // depth
    return pl.pallas_call(
        functools.partial(partial_kernel, steps),
        grid=(steps,),
        out_shape=jax.ShapeDtypeStruct((GRID, count, width), kind),
        in_specs=[
            pl.BlockSpec((count, depth), lambda i: (0, i)),
            pl.BlockSpec((depth, width), lambda i: (i, 0)),
            pl.BlockSpec((2 * GRID, depth, LANES), lambda i: (0, i, 0)),
        ],
        out_specs=pl.BlockSpec((GRID, count, width), lambda i: (0, 0, 0)),
        scratch_shapes=[
            pltpu.VMEM((GRID, count, width), jnp.float32),
            pltpu.VMEM((GRID, depth, min(TILE, -(-width // LANES) * LANES)), jnp.bfloat16),
        ],
        compiler_params=pltpu.CompilerParams(
            dimension_semantics=("arbitrary",), vmem_limit_bytes=48 << 20
        ),
        cost_estimate=pl.CostEstimate(
            flops=30 * GRID * channels * width * 16,
            bytes_accessed=4 * channels * width,
            transcendentals=0,
        ),
    )(tokens, columns, table)


def in_halves(activations, weight):
    n = lax.axis_size("dp")
    half = n // 2
    me = lax.axis_index("dp")
    side, place = me // half, me % half
    groups = [list(range(half)), list(range(half, n))]
    across = [(i, (i + half) % n) for i in range(n)]

    widened = lax.all_gather(activations, "tensor", axis=1, tiled=True)
    own_tokens, channels = widened.shape
    mine = channels // 2
    token_count = own_tokens * n
    kept = lax.dynamic_slice_in_dim(widened, side * mine, mine, axis=1)
    away = lax.dynamic_slice_in_dim(widened, (1 - side) * mine, mine, axis=1)
    other = lax.ppermute(away, "dp", across)
    first = side == 0
    pair = jnp.concatenate([jnp.where(first, kept, other), jnp.where(first, other, kept)], axis=0)
    tokens = lax.all_gather(pair, "dp", axis=0, tiled=True, axis_index_groups=groups)

    width = weight.shape[1]
    away_weight = lax.dynamic_slice_in_dim(weight, (1 - side) * (width // 2), width // 2, axis=1)
    kept_weight = lax.dynamic_slice_in_dim(weight, side * (width // 2), width // 2, axis=1)
    exchange = functools.partial(
        lax.all_to_all, axis_name="dp", split_axis=1, concat_axis=0, tiled=True, axis_index_groups=groups
    )
    away_columns = exchange(away_weight)
    kept_columns = exchange(kept_weight)

    half_mean = jnp.sum(jnp.abs(tokens.astype(jnp.float32)), axis=0) / token_count + 1e-06
    other_mean = lax.ppermute(half_mean, "dp", across)
    ratios = jnp.arange(GRID, dtype=jnp.float32) / GRID
    raw = jnp.exp(ratios[:, None] * jnp.log(half_mean)[None, :])
    raw_other = jnp.exp(ratios[:, None] * jnp.log(other_mean)[None, :])
    top = jnp.maximum(jnp.max(raw, axis=1, keepdims=True), jnp.max(raw_other, axis=1, keepdims=True))
    bottom = jnp.minimum(jnp.min(raw, axis=1, keepdims=True), jnp.min(raw_other, axis=1, keepdims=True))
    scales = raw / jnp.sqrt(top * bottom)
    table = jnp.concatenate([scales, 1.0 / scales], axis=0)
    table = jnp.broadcast_to(table[:, :, None], (2 * GRID, mine, LANES))

    depth = weight.shape[0]
    away_part = partial_residue(tokens, away_columns, table, depth, jnp.bfloat16)
    arrived = lax.ppermute(away_part, "dp", across)
    own_part = partial_residue(tokens, kept_columns, table, depth, jnp.float32)
    residue = own_part + arrived.astype(jnp.float32)
    column_sums = jnp.sum(residue * residue, axis=1)

    totals = lax.psum(jnp.sum(column_sums, axis=1), ("dp", "tensor"))
    errors = totals / (token_count * width * lax.axis_size("tensor"))
    column_errors = column_sums / token_count
    own_mean = lax.dynamic_slice_in_dim(half_mean, place * depth, depth)
    return (own_mean, column_errors, errors)


PLANES = 4
CHUNK = LANES
BLOCK = 512
AHEAD = 4
SKEW = 3
EARLY = 4
BOW = (12.568868617017895, 50.02489230906822, 77.93933755195671)
BOW_SHIFT = BOW[1] / (2.0 * BOW[2])
BOW_FLOOR = BOW[0] / BOW[2] - BOW_SHIFT * BOW_SHIFT


def change_of(w16, scale, unscale):
    w = w16.astype(jnp.float32)
    scaled = w if scale is None else w * scale
    top = jnp.max(jnp.abs(scaled), axis=0, keepdims=True) + 1e-06
    v = scaled * (7.0 / top)
    r = v - jnp.round(v)
    size = jnp.abs(r)
    rest = 0.5 - size
    m = size * rest + BOW_SHIFT
    wave = (r * rest) * (m * m + BOW_FLOOR) * (top * (BOW[2] / (14.0 * math.pi)))
    if unscale is not None:
        wave = wave * unscale
    return (w - wave).astype(jnp.bfloat16) - w16


def fused_kernel(
    n, a_ref, w_ref, mean_ref, col_ref, err_ref,
    wbuf, abuf, astage, table, meanrow, change, acc, stage, recv, colsum, cbuf, mine, theirs, etile, etiles, ztile, ztiles, inward,
    w_send, w_recv, az_send, az_recv, ab_send, ab_recv, mm_send, mm_recv, p_send, p_recv, c_send, c_recv, e_send, e_recv, t_send, t_recv, i_send, i_recv,
):
    depth = w_ref.shape[0]
    plane = n // PLANES
    channels = plane * depth
    chunks = wbuf.shape[0]
    half, per = chunks // 2, chunks // PLANES
    tokens = abuf.shape[0]
    own = tokens // n
    rows_each = own * PLANES
    me = lax.axis_index("dp")
    z, p = me // plane, me % plane
    partner = p + 1 - 2 * (p % 2)

    def copy_to(device, source, target, send, arrive):
        return pltpu.make_async_remote_copy(
            src_ref=source, dst_ref=target, send_sem=send, recv_sem=arrive,
            device_id={"dp": device}, device_id_type=pl.DeviceIdType.MESH,
        )

    def settle(ref, sem):
        pltpu.make_async_copy(ref, ref, sem).wait()

    barrier = pltpu.get_barrier_semaphore()

    near = [z * plane + (p + j) % plane for j in range(1, plane)]
    near += [(z + i) % PLANES * plane + p for i in range(1, PLANES)]
    for device in near:
        pl.semaphore_signal(barrier, inc=1, device_id={"dp": device}, device_id_type=pl.DeviceIdType.MESH)
    pl.semaphore_wait(barrier, len(near))

    def slab(at):
        return a_ref.at[:, pl.ds(pl.multiple_of(at * channels, channels), channels)]

    def z_copy(i):
        to = (z + i) % PLANES
        return copy_to(to * plane + p, slab(to), astage.at[z], az_send.at[i], az_recv.at[z])

    for i in range(1, PLANES):
        z_copy(i).start()
    pltpu.make_async_copy(slab(z), astage.at[z], az_recv.at[z]).start()

    lead = jnp.where(z < PLANES // 2, 1, 0)
    skew = jnp.where((z == 0) | (z == PLANES - 1), SKEW, 0)

    def place_of(side, index):
        return jnp.where(side == 0, index, chunks - 1 - index)

    def swapped(step, when):
        return jnp.where(when & (step == chunks - 3), chunks - 2,
                         jnp.where(when & (step == chunks - 2), chunks - 3, step))

    def chunk_of(step):
        step = swapped(step, skew == 0)
        early = step <= skew
        late = step >= chunks - 1 - skew
        even = (step + skew) % 2 == 0
        side = jnp.where(early | (even & jnp.logical_not(late)), lead, 1 - lead)
        middle = jnp.where(even, (step + skew) // 2, (step + chunks - skew - 1) // 2 - half)
        index = jnp.where(early, step, jnp.where(late, step - half, middle))
        moved = (skew > 0) & (side != lead) & (index >= half - EARLY)
        index = jnp.where(moved, jnp.where(index == half - EARLY, half - 1, index - 1), index)
        return place_of(side, index)

    def send_weights(step):
        c = chunk_of(step)
        rows = pl.ds(pl.multiple_of(p * depth, depth), depth)

        def piece(q):
            at = pl.multiple_of(((c // per) * plane * per + q * per + c % per) * CHUNK, CHUNK)
            return w_ref.at[:, pl.ds(at, CHUNK)]

        @pl.loop(1, plane)
        def _(j):
            q = (p + j) % plane
            copy_to(z * plane + q, piece(q), wbuf.at[c, rows, :], w_send.at[c], w_recv.at[c]).start()

        pltpu.make_async_copy(piece(p), wbuf.at[c, rows, :], w_recv.at[c]).start()

    send_weights(0)

    for i in range(PLANES):
        settle(astage.at[i], az_recv.at[i])

    def block(q):
        return abuf.at[pl.ds(pl.multiple_of(q * rows_each, rows_each), rows_each), :]

    @pl.loop(0, channels // LANES)
    def _(i):
        lanes = pl.ds(pl.multiple_of(i * LANES, LANES), LANES)
        part = [astage[t, :, lanes].astype(jnp.float32) for t in range(PLANES)]
        whole = jnp.concatenate(part, axis=0).astype(jnp.bfloat16)
        abuf[pl.ds(pl.multiple_of(p * rows_each, rows_each), rows_each), lanes] = whole

    for j in range(1, plane // 2):
        to = (p + 2 * j) % plane
        copy_to(z * plane + to, block(p), block(p), ab_send.at[j], ab_recv.at[p]).start()
    copy_to(z * plane + partner, block(p), block(p), ab_send.at[0], ab_recv.at[p]).start()

    for step in range(1, AHEAD):
        send_weights(step)

    for j in range(1, plane // 2):
        q = (p + 2 * j) % plane
        settle(block(q), ab_recv.at[q])
        copy_to(z * plane + partner, block(q), block(q), ab_send.at[plane // 2 + j - 1], ab_recv.at[q]).start()
    for j in range(plane // 2):
        q = (partner + 2 * j) % plane
        settle(block(q), ab_recv.at[q])

    def means(i, carry):
        most, least = carry
        lanes = pl.ds(pl.multiple_of(i * LANES, LANES), LANES)
        sums = jnp.sum(jnp.abs(abuf[:, lanes].astype(jnp.float32)), axis=0, keepdims=True)
        mean = sums / tokens + 1e-06
        meanrow[:, lanes] = mean
        table[0, lanes, :] = jnp.transpose(jnp.broadcast_to(jnp.log(mean), (LANES, LANES)))
        return jnp.maximum(most, mean), jnp.minimum(least, mean)

    most, least = lax.fori_loop(
        0, channels // LANES, means,
        (jnp.zeros((1, LANES), jnp.float32), jnp.full((1, LANES), jnp.inf, jnp.float32)),
    )
    mean_ref[...] = meanrow[:, pl.ds(pl.multiple_of(p * depth, depth), depth)]
    mine[0:1, :] = most
    mine[1:2, :] = least

    def mm_copy(i):
        to = (z + i) % PLANES
        return copy_to(to * plane + p, mine, theirs.at[i], mm_send.at[i], mm_recv.at[i])

    for i in range(1, PLANES):
        mm_copy(i).start()
    for i in range(1, PLANES):
        settle(theirs.at[i], mm_recv.at[i])
        most = jnp.maximum(most, theirs[i, 0:1, :])
        least = jnp.minimum(least, theirs[i, 1:2, :])
    ends = jnp.log(jnp.max(most, axis=1, keepdims=True)) + jnp.log(jnp.min(least, axis=1, keepdims=True))
    middle = 0.5 * ends

    @pl.loop(0, channels // LANES)
    def _(i):
        rows = pl.ds(pl.multiple_of(i * LANES, LANES), LANES)
        level = table[0, rows, :] - middle
        for k in range(1, GRID):
            table[2 * k - 2, rows, :] = jnp.exp((k / GRID) * level)
            table[2 * k - 1, rows, :] = jnp.exp((-k / GRID) * level)

    def add_product(pair, base):
        lhs = abuf[:, pl.ds(base, BLOCK)]
        acc[pair] += jnp.dot(lhs, change[pair], preferred_element_type=jnp.float32)

    def partial_products(c):
        acc[...] = jnp.zeros_like(acc)
        change[1] = jnp.zeros_like(change[1])

        @pl.loop(0, channels // BLOCK)
        def _(b):
            base = pl.multiple_of(b * BLOCK, BLOCK)
            add_product(1, pl.multiple_of(jnp.maximum(base - BLOCK, 0), BLOCK))
            for pair in range(GRID // 2):
                for k in (2 * pair, 2 * pair + 1):
                    for g in range(BLOCK // GROUP):
                        rows = pl.ds(base + g * GROUP, GROUP)
                        scale = table[2 * k - 2, rows, :] if k else None
                        unscale = table[2 * k - 1, rows, :] if k else None
                        change[pair, pl.ds(g * GROUP, GROUP), pl.ds(k % 2 * CHUNK, CHUNK)] = change_of(
                            wbuf[c, rows, :], scale, unscale
                        )
                if pair == 0:
                    add_product(0, base)

        add_product(1, channels - BLOCK)

    def hand_inward(c, k, to):
        return copy_to(to * plane + p, stage.at[c, k], inward.at[k], i_send.at[k], i_recv.at[k])

    def hand_on(c, k, to):
        return copy_to(to * plane + p, stage.at[c, k], recv.at[c, k], p_send.at[c, k], p_recv.at[c, k])

    steps = chunks
    for_side = ((PLANES - 1 - z, z - 1), (z, z + 1))
    last_of = (half - 1, half)

    colsum[...] = jnp.zeros_like(colsum)

    @pl.loop(0, steps - 1 + 2 * (PLANES - 2))
    def _(step):
        @pl.when(step < steps)
        def _():
            c = chunk_of(step)

            @pl.when(step + AHEAD < steps)
            def _():
                send_weights(step + AHEAD)

            settle(wbuf.at[c], w_recv.at[c])
            partial_products(c)
            for k in range(GRID):
                stage[c, k] = acc[k // 2, :, k % 2 * CHUNK : (k % 2 + 1) * CHUNK].astype(jnp.bfloat16)
            for side in range(2):
                gone, to = for_side[side]

                @pl.when((c // half == side) & (gone == 0))
                def _():
                    for k in range(GRID):
                        hand_on(c, k, to).start()

                @pl.when((c == last_of[side]) & (gone == PLANES - 1))
                def _():
                    for k in range(GRID):
                        hand_inward(c, k, z + (1 - 2 * side)).start()

        for side in range(2):
            gone, to = for_side[side]
            turn = step - 2 * (gone - 1) - jnp.where(gone == PLANES - 1, 2, 0)
            turn = swapped(turn, gone == 1)
            index = jnp.where(turn < 4, turn - 2, turn // 2)
            c = place_of(side, index)
            inner_end = (index == half - 1) & (gone == PLANES - 2)
            due = (turn % 2 == 0) | (turn < 4)
            ready = (gone > 0) & (turn >= 2) & due & (index < half)

            @pl.when(ready & (gone < PLANES - 1) & jnp.logical_not(inner_end))
            def _():
                for k in range(GRID):
                    settle(recv.at[c, k], p_recv.at[c, k])
                    total = stage[c, k].astype(jnp.float32) + recv[c, k].astype(jnp.float32)
                    stage[c, k] = total.astype(jnp.bfloat16)
                    hand_on(c, k, to).start()

            def finish(extra):
                for k in range(GRID):
                    settle(recv.at[c, k], p_recv.at[c, k])
                    residue = stage[c, k].astype(jnp.float32) + recv[c, k].astype(jnp.float32)
                    if extra:
                        settle(inward.at[k], i_recv.at[k])
                        residue += inward[k].astype(jnp.float32)
                    sums = jnp.sum(residue * residue, axis=0, keepdims=True)
                    lanes = pl.ds(pl.multiple_of(c % per * CHUNK, CHUNK), CHUNK)
                    colsum[c // per, k : k + 1, lanes] = sums

            @pl.when(ready & (gone == PLANES - 1) & (index < half - 1))
            def _():
                finish(False)

            @pl.when(ready & inner_end)
            def _():
                finish(True)

    outer = (z == 0) | (z == PLANES - 1)
    inner = jnp.where(z == 0, 1, PLANES - 2)

    def column_copy():
        return copy_to(inner * plane + p, colsum.at[inner], cbuf, c_send, c_recv)

    def total_copy(j):
        return copy_to(z * plane + (p + j) % plane, etile, etiles.at[p], e_send.at[j], e_recv.at[p])

    def line_copy(i):
        return copy_to((z + i) % PLANES * plane + p, ztile, ztiles.at[z], t_send.at[i], t_recv.at[z])

    @pl.when(outer)
    def _():
        column_copy().start()

    total = jnp.zeros((8, 1), jnp.float32)
    for i in range(PLANES):
        total += jnp.sum(colsum[i], axis=1, keepdims=True)
    etile[...] = jnp.broadcast_to(total, (8, LANES))
    for j in range(1, plane):
        total_copy(j).start()
    etiles[p] = etile[...]
    for j in range(1, plane):
        q = (p + j) % plane
        settle(etiles.at[q], e_recv.at[q])
    total = etiles[0]
    for q in range(1, plane):
        total += etiles[q]
    ztile[...] = total
    for i in range(1, PLANES):
        line_copy(i).start()
    ztiles[z] = total

    @pl.when(outer)
    def _():
        col_ref[...] = colsum[z] * (1.0 / tokens)

    @pl.when(jnp.logical_not(outer))
    def _():
        settle(cbuf, c_recv)
        col_ref[...] = (colsum[z] + cbuf[...]) * (1.0 / tokens)

    for i in range(1, PLANES):
        settle(ztiles.at[(z + i) % PLANES], t_recv.at[(z + i) % PLANES])
    total = ztiles[0]
    for i in range(1, PLANES):
        total += ztiles[i]
    on_lane = lax.broadcasted_iota(jnp.int32, (8, LANES), 0) == lax.broadcasted_iota(jnp.int32, (8, LANES), 1)
    err_ref[...] = jnp.sum(jnp.where(on_lane, total, 0.0), axis=0, keepdims=True) * (
        1.0 / (tokens * plane * chunks * CHUNK)
    )

    for i in range(1, PLANES):
        z_copy(i).wait_send()
        mm_copy(i).wait_send()
    for i in range(plane - 1):
        settle(block(0), ab_send.at[i])

    @pl.loop(0, chunks)
    def _(c):
        settle(wbuf.at[0, pl.ds(0, channels - depth), :], w_send.at[c])

        for side in range(2):
            gone, to = for_side[side]

            passed_on = (c // half == side) & (gone < PLANES - 1)
            inner_end = (c == last_of[side]) & (gone == PLANES - 2)

            @pl.when(passed_on & jnp.logical_not(inner_end))
            def _():
                for k in range(GRID):
                    settle(stage.at[c, k], p_send.at[c, k])

    @pl.when(outer)
    def _():
        for k in range(GRID):
            settle(stage.at[0, k], i_send.at[k])
        settle(cbuf, c_send)

    for j in range(1, plane):
        settle(etile, e_send.at[j])
    for i in range(1, PLANES):
        settle(ztile, t_send.at[i])


def shape_results(mean_in, col_in, err_in, mean_ref, col_ref, err_ref):
    mean_ref[...] = mean_in[0, :]
    col_ref[...] = col_in[:GRID, :]
    err_ref[...] = err_in[0, :GRID]


def in_one_kernel(activations, weight):
    n = lax.axis_size("dp")
    own, depth = activations.shape[0], weight.shape[0]
    plane = n // PLANES
    channels, tokens = plane * depth, n * own
    chunks = weight.shape[1] // (plane * CHUNK)
    width = weight.shape[1] // n
    dma, f32, bf16 = pltpu.SemaphoreType.DMA, jnp.float32, jnp.bfloat16
    mean, columns, errors = pl.pallas_call(
        functools.partial(fused_kernel, n),
        out_shape=(
            jax.ShapeDtypeStruct((1, depth), f32),
            jax.ShapeDtypeStruct((8, width), f32),
            jax.ShapeDtypeStruct((1, LANES), f32),
        ),
        in_specs=[pl.BlockSpec(memory_space=pl.ANY)] * 2,
        out_specs=[pl.BlockSpec(memory_space=pltpu.VMEM)] * 3,
        scratch_shapes=[
            pltpu.VMEM((chunks, channels, CHUNK), bf16),
            pltpu.VMEM((tokens, channels), bf16),
            pltpu.VMEM((PLANES, own, channels), bf16),
            pltpu.VMEM((2 * GRID - 2, channels, LANES), f32),
            pltpu.VMEM((1, channels), f32),
            pltpu.VMEM((GRID // 2, BLOCK, 2 * CHUNK), bf16),
            pltpu.VMEM((GRID // 2, tokens, 2 * CHUNK), f32),
            pltpu.VMEM((chunks, GRID, tokens, CHUNK), bf16),
            pltpu.VMEM((chunks, GRID, tokens, CHUNK), bf16),
            pltpu.VMEM((PLANES, 8, width), f32),
            pltpu.VMEM((8, width), f32),
            pltpu.VMEM((8, LANES), f32),
            pltpu.VMEM((PLANES, 8, LANES), f32),
            pltpu.VMEM((8, LANES), f32),
            pltpu.VMEM((plane, 8, LANES), f32),
            pltpu.VMEM((8, LANES), f32),
            pltpu.VMEM((PLANES, 8, LANES), f32),
            pltpu.VMEM((GRID, tokens, CHUNK), bf16),
            dma((chunks,)), dma((chunks,)),
            dma((PLANES,)), dma((PLANES,)),
            dma((plane,)), dma((plane,)),
            dma((PLANES,)), dma((PLANES,)),
            dma((chunks, GRID)), dma((chunks, GRID)),
            dma, dma,
            dma((plane,)), dma((plane,)),
            dma((PLANES,)), dma((PLANES,)),
            dma((GRID,)), dma((GRID,)),
        ],
        compiler_params=pltpu.CompilerParams(
            collective_id=0, has_side_effects=True, vmem_limit_bytes=62 << 20
        ),
    )(activations, weight)
    return pl.pallas_call(
        shape_results,
        out_shape=(
            jax.ShapeDtypeStruct((depth,), f32),
            jax.ShapeDtypeStruct((GRID, width), f32),
            jax.ShapeDtypeStruct((GRID,), f32),
        ),
        in_specs=[pl.BlockSpec(memory_space=pltpu.VMEM)] * 3,
        out_specs=[pl.BlockSpec(memory_space=pltpu.VMEM)] * 3,
    )(mean, columns, errors)


def one_kernel_fits(activations, weight):
    n, tensor = lax.axis_size("dp"), lax.axis_size("tensor")
    if tensor != 1 or n % (2 * PLANES) or n < 4 * PLANES:
        return False
    plane = n // PLANES
    channels, width = plane * weight.shape[0], weight.shape[1]
    aligned = (activations.shape[0] * PLANES) % 16 == 0 and weight.shape[0] % GROUP == 0
    return aligned and channels % BLOCK == 0 and width % (CHUNK * n) == 0


def on_device(activations, weight):
    if one_kernel_fits(activations, weight):
        return in_one_kernel(activations, weight)
    return in_halves(activations, weight)


def solution(mesh):
    placed = (P("dp", "tensor"), P("dp", "tensor"))
    return jax.shard_map(
        on_device,
        mesh=mesh,
        in_specs=placed,
        out_specs=(P("dp"), P(None, ("tensor", "dp")), P()),
        check_vma=False,
    )
```

```python
import functools
import math

import jax
import jax.numpy as jnp
from jax import lax
from jax.experimental import pallas as pl
from jax.experimental.pallas import tpu as pltpu
from jax.sharding import PartitionSpec as P

GROUP = 128
GRID = 4
LANES = 128
TILE = 256
SINE = (
    6.283182818832115,
    -41.34142141640176,
    81.59618421926638,
    -76.5801034177733,
    41.205405703161745,
    -12.271277356143528,
)


def sine_of_turns(r):
    square = r * r
    value = SINE[-1] * square + SINE[-2]
    for c in SINE[-3::-1]:
        value = value * square + c
    return value * r


def partial_kernel(steps, a_ref, w_ref, s_ref, out_ref, acc, change):
    step = pl.program_id(0)
    depth, width = w_ref.shape

    @pl.when(step == 0)
    def _():
        acc[...] = jnp.zeros_like(acc)

    def tile(start, size):
        def columns(offset, length):
            if isinstance(start, int):
                return pl.ds(start + offset, length)
            return pl.ds(pl.multiple_of(start + offset, LANES), length)

        for k in range(GRID):
            for g in range(depth // GROUP):
                rows = pl.ds(g * GROUP, GROUP)
                for c in range(0, size, LANES):
                    lanes = min(LANES, size - c)
                    w = w_ref[rows, columns(c, lanes)].astype(jnp.float32)
                    scaled = w * s_ref[k, rows, :lanes]
                    top = jnp.max(jnp.abs(scaled), axis=0, keepdims=True)
                    quant_step = (top + 1e-06) / 7.0
                    v = scaled * (1.0 / quant_step)
                    wave = sine_of_turns(v - jnp.round(v))
                    wave = wave * (quant_step * (0.5 / math.pi))
                    dequant = w - wave * s_ref[GRID + k, rows, :lanes]
                    dequant = dequant.astype(jnp.bfloat16).astype(jnp.float32)
                    change[k, rows, pl.ds(c, lanes)] = (dequant - w).astype(jnp.bfloat16)
            acc[k, :, columns(0, size)] += jnp.dot(
                a_ref[...], change[k, :, pl.ds(0, size)], preferred_element_type=jnp.float32
            )

    whole = width // TILE
    if whole:

        @pl.loop(0, whole)
        def _(i):
            tile(i * TILE, TILE)

    if width % TILE:
        tile(whole * TILE, width % TILE)

    @pl.when(step == steps - 1)
    def _():
        for k in range(GRID):
            out_ref[k] = acc[k].astype(out_ref.dtype)


def partial_residue(tokens, columns, table, depth, kind):
    count, channels = tokens.shape
    width = columns.shape[1]
    steps = channels // depth
    return pl.pallas_call(
        functools.partial(partial_kernel, steps),
        grid=(steps,),
        out_shape=jax.ShapeDtypeStruct((GRID, count, width), kind),
        in_specs=[
            pl.BlockSpec((count, depth), lambda i: (0, i)),
            pl.BlockSpec((depth, width), lambda i: (i, 0)),
            pl.BlockSpec((2 * GRID, depth, LANES), lambda i: (0, i, 0)),
        ],
        out_specs=pl.BlockSpec((GRID, count, width), lambda i: (0, 0, 0)),
        scratch_shapes=[
            pltpu.VMEM((GRID, count, width), jnp.float32),
            pltpu.VMEM((GRID, depth, min(TILE, -(-width // LANES) * LANES)), jnp.bfloat16),
        ],
        compiler_params=pltpu.CompilerParams(
            dimension_semantics=("arbitrary",), vmem_limit_bytes=48 << 20
        ),
        cost_estimate=pl.CostEstimate(
            flops=30 * GRID * channels * width * 16,
            bytes_accessed=4 * channels * width,
            transcendentals=0,
        ),
    )(tokens, columns, table)


def in_halves(activations, weight):
    n = lax.axis_size("dp")
    half = n // 2
    me = lax.axis_index("dp")
    side, place = me // half, me % half
    groups = [list(range(half)), list(range(half, n))]
    across = [(i, (i + half) % n) for i in range(n)]

    widened = lax.all_gather(activations, "tensor", axis=1, tiled=True)
    own_tokens, channels = widened.shape
    mine = channels // 2
    token_count = own_tokens * n
    kept = lax.dynamic_slice_in_dim(widened, side * mine, mine, axis=1)
    away = lax.dynamic_slice_in_dim(widened, (1 - side) * mine, mine, axis=1)
    other = lax.ppermute(away, "dp", across)
    first = side == 0
    pair = jnp.concatenate([jnp.where(first, kept, other), jnp.where(first, other, kept)], axis=0)
    tokens = lax.all_gather(pair, "dp", axis=0, tiled=True, axis_index_groups=groups)

    width = weight.shape[1]
    away_weight = lax.dynamic_slice_in_dim(weight, (1 - side) * (width // 2), width // 2, axis=1)
    kept_weight = lax.dynamic_slice_in_dim(weight, side * (width // 2), width // 2, axis=1)
    exchange = functools.partial(
        lax.all_to_all, axis_name="dp", split_axis=1, concat_axis=0, tiled=True, axis_index_groups=groups
    )
    away_columns = exchange(away_weight)
    kept_columns = exchange(kept_weight)

    half_mean = jnp.sum(jnp.abs(tokens.astype(jnp.float32)), axis=0) / token_count + 1e-06
    other_mean = lax.ppermute(half_mean, "dp", across)
    ratios = jnp.arange(GRID, dtype=jnp.float32) / GRID
    raw = jnp.exp(ratios[:, None] * jnp.log(half_mean)[None, :])
    raw_other = jnp.exp(ratios[:, None] * jnp.log(other_mean)[None, :])
    top = jnp.maximum(jnp.max(raw, axis=1, keepdims=True), jnp.max(raw_other, axis=1, keepdims=True))
    bottom = jnp.minimum(jnp.min(raw, axis=1, keepdims=True), jnp.min(raw_other, axis=1, keepdims=True))
    scales = raw / jnp.sqrt(top * bottom)
    table = jnp.concatenate([scales, 1.0 / scales], axis=0)
    table = jnp.broadcast_to(table[:, :, None], (2 * GRID, mine, LANES))

    depth = weight.shape[0]
    away_part = partial_residue(tokens, away_columns, table, depth, jnp.bfloat16)
    arrived = lax.ppermute(away_part, "dp", across)
    own_part = partial_residue(tokens, kept_columns, table, depth, jnp.float32)
    residue = own_part + arrived.astype(jnp.float32)
    column_sums = jnp.sum(residue * residue, axis=1)

    totals = lax.psum(jnp.sum(column_sums, axis=1), ("dp", "tensor"))
    errors = totals / (token_count * width * lax.axis_size("tensor"))
    column_errors = column_sums / token_count
    own_mean = lax.dynamic_slice_in_dim(half_mean, place * depth, depth)
    return (own_mean, column_errors, errors)


PLANES = 4
CHUNK = LANES
BLOCK = 512
AHEAD = 4
SKEW = 3
EARLY = 4
BOW = (12.568868617017895, 50.02489230906822, 77.93933755195671)
BOW_SHIFT = BOW[1] / (2.0 * BOW[2])
BOW_FLOOR = BOW[0] / BOW[2] - BOW_SHIFT * BOW_SHIFT


def change_of(w16, scale, unscale):
    w = w16.astype(jnp.float32)
    scaled = w if scale is None else w * scale
    top = jnp.max(jnp.abs(scaled), axis=0, keepdims=True) + 1e-06
    v = scaled * (7.0 / top)
    r = v - jnp.round(v)
    size = jnp.abs(r)
    rest = 0.5 - size
    m = size * rest + BOW_SHIFT
    wave = (r * rest) * (m * m + BOW_FLOOR) * (top * (BOW[2] / (14.0 * math.pi)))
    if unscale is not None:
        wave = wave * unscale
    return (w - wave).astype(jnp.bfloat16) - w16


def fused_kernel(
    n, a_ref, w_ref, mean_ref, col_ref, err_ref,
    wbuf, abuf, astage, table, meanrow, change, acc, stage, recv, colsum, cbuf, mine, theirs, etile, etiles, ztile, ztiles, inward,
    w_send, w_recv, az_send, az_recv, ab_send, ab_recv, mm_send, mm_recv, p_send, p_recv, c_send, c_recv, e_send, e_recv, t_send, t_recv, i_send, i_recv,
):
    depth = w_ref.shape[0]
    plane = n // PLANES
    channels = plane * depth
    chunks = wbuf.shape[0]
    half, per = chunks // 2, chunks // PLANES
    tokens = abuf.shape[0]
    own = tokens // n
    rows_each = own * PLANES
    me = lax.axis_index("dp")
    z, p = me // plane, me % plane
    partner = p + 1 - 2 * (p % 2)

    def copy_to(device, source, target, send, arrive):
        return pltpu.make_async_remote_copy(
            src_ref=source, dst_ref=target, send_sem=send, recv_sem=arrive,
            device_id={"dp": device}, device_id_type=pl.DeviceIdType.MESH,
        )

    def settle(ref, sem):
        pltpu.make_async_copy(ref, ref, sem).wait()

    barrier = pltpu.get_barrier_semaphore()

    near = [z * plane + (p + j) % plane for j in range(1, plane)]
    near += [(z + i) % PLANES * plane + p for i in range(1, PLANES)]
    for device in near:
        pl.semaphore_signal(barrier, inc=1, device_id={"dp": device}, device_id_type=pl.DeviceIdType.MESH)
    pl.semaphore_wait(barrier, len(near))

    def slab(at):
        return a_ref.at[:, pl.ds(pl.multiple_of(at * channels, channels), channels)]

    def z_copy(i):
        to = (z + i) % PLANES
        return copy_to(to * plane + p, slab(to), astage.at[z], az_send.at[i], az_recv.at[z])

    for i in range(1, PLANES):
        z_copy(i).start()
    pltpu.make_async_copy(slab(z), astage.at[z], az_recv.at[z]).start()

    lead = jnp.where(z < PLANES // 2, 1, 0)
    skew = jnp.where((z == 0) | (z == PLANES - 1), SKEW, 0)

    def place_of(side, index):
        return jnp.where(side == 0, index, chunks - 1 - index)

    def swapped(step, when):
        return jnp.where(when & (step == chunks - 3), chunks - 2,
                         jnp.where(when & (step == chunks - 2), chunks - 3, step))

    def chunk_of(step):
        step = swapped(step, skew == 0)
        early = step <= skew
        late = step >= chunks - 1 - skew
        even = (step + skew) % 2 == 0
        side = jnp.where(early | (even & jnp.logical_not(late)), lead, 1 - lead)
        middle = jnp.where(even, (step + skew) // 2, (step + chunks - skew - 1) // 2 - half)
        index = jnp.where(early, step, jnp.where(late, step - half, middle))
        moved = (skew > 0) & (side != lead) & (index >= half - EARLY)
        index = jnp.where(moved, jnp.where(index == half - EARLY, half - 1, index - 1), index)
        return place_of(side, index)

    def send_weights(step):
        c = chunk_of(step)
        rows = pl.ds(pl.multiple_of(p * depth, depth), depth)

        def piece(q):
            at = pl.multiple_of(((c // per) * plane * per + q * per + c % per) * CHUNK, CHUNK)
            return w_ref.at[:, pl.ds(at, CHUNK)]

        @pl.loop(1, plane)
        def _(j):
            q = (p + j) % plane
            copy_to(z * plane + q, piece(q), wbuf.at[c, rows, :], w_send.at[c], w_recv.at[c]).start()

        pltpu.make_async_copy(piece(p), wbuf.at[c, rows, :], w_recv.at[c]).start()

    send_weights(0)

    for i in range(PLANES):
        settle(astage.at[i], az_recv.at[i])

    def block(q):
        return abuf.at[pl.ds(pl.multiple_of(q * rows_each, rows_each), rows_each), :]

    @pl.loop(0, channels // LANES)
    def _(i):
        lanes = pl.ds(pl.multiple_of(i * LANES, LANES), LANES)
        part = [astage[t, :, lanes].astype(jnp.float32) for t in range(PLANES)]
        whole = jnp.concatenate(part, axis=0).astype(jnp.bfloat16)
        abuf[pl.ds(pl.multiple_of(p * rows_each, rows_each), rows_each), lanes] = whole

    for j in range(1, plane // 2):
        to = (p + 2 * j) % plane
        copy_to(z * plane + to, block(p), block(p), ab_send.at[j], ab_recv.at[p]).start()
    copy_to(z * plane + partner, block(p), block(p), ab_send.at[0], ab_recv.at[p]).start()

    for step in range(1, AHEAD):
        send_weights(step)

    for j in range(1, plane // 2):
        q = (p + 2 * j) % plane
        settle(block(q), ab_recv.at[q])
        copy_to(z * plane + partner, block(q), block(q), ab_send.at[plane // 2 + j - 1], ab_recv.at[q]).start()
    for j in range(plane // 2):
        q = (partner + 2 * j) % plane
        settle(block(q), ab_recv.at[q])

    def means(i, carry):
        most, least = carry
        lanes = pl.ds(pl.multiple_of(i * LANES, LANES), LANES)
        sums = jnp.sum(jnp.abs(abuf[:, lanes].astype(jnp.float32)), axis=0, keepdims=True)
        mean = sums / tokens + 1e-06
        meanrow[:, lanes] = mean
        table[0, lanes, :] = jnp.transpose(jnp.broadcast_to(jnp.log(mean), (LANES, LANES)))
        return jnp.maximum(most, mean), jnp.minimum(least, mean)

    most, least = lax.fori_loop(
        0, channels // LANES, means,
        (jnp.zeros((1, LANES), jnp.float32), jnp.full((1, LANES), jnp.inf, jnp.float32)),
    )
    mean_ref[...] = meanrow[:, pl.ds(pl.multiple_of(p * depth, depth), depth)]
    mine[0:1, :] = most
    mine[1:2, :] = least

    def mm_copy(i):
        to = (z + i) % PLANES
        return copy_to(to * plane + p, mine, theirs.at[i], mm_send.at[i], mm_recv.at[i])

    for i in range(1, PLANES):
        mm_copy(i).start()
    for i in range(1, PLANES):
        settle(theirs.at[i], mm_recv.at[i])
        most = jnp.maximum(most, theirs[i, 0:1, :])
        least = jnp.minimum(least, theirs[i, 1:2, :])
    ends = jnp.log(jnp.max(most, axis=1, keepdims=True)) + jnp.log(jnp.min(least, axis=1, keepdims=True))
    middle = 0.5 * ends

    @pl.loop(0, channels // LANES)
    def _(i):
        rows = pl.ds(pl.multiple_of(i * LANES, LANES), LANES)
        level = table[0, rows, :] - middle
        for k in range(1, GRID):
            table[2 * k - 2, rows, :] = jnp.exp((k / GRID) * level)
            table[2 * k - 1, rows, :] = jnp.exp((-k / GRID) * level)

    def add_product(pair, base):
        lhs = abuf[:, pl.ds(base, BLOCK)]
        acc[pair] += jnp.dot(lhs, change[pair], preferred_element_type=jnp.float32)

    def partial_products(c):
        acc[...] = jnp.zeros_like(acc)
        change[1] = jnp.zeros_like(change[1])

        @pl.loop(0, channels // BLOCK)
        def _(b):
            base = pl.multiple_of(b * BLOCK, BLOCK)
            add_product(1, pl.multiple_of(jnp.maximum(base - BLOCK, 0), BLOCK))
            for pair in range(GRID // 2):
                for g in range(BLOCK // GROUP):
                    for k in (2 * pair, 2 * pair + 1):
                        rows = pl.ds(base + g * GROUP, GROUP)
                        scale = table[2 * k - 2, rows, :] if k else None
                        unscale = table[2 * k - 1, rows, :] if k else None
                        change[pair, pl.ds(g * GROUP, GROUP), pl.ds(k % 2 * CHUNK, CHUNK)] = change_of(
                            wbuf[c, rows, :], scale, unscale
                        )
                if pair == 0:
                    add_product(0, base)

        add_product(1, channels - BLOCK)

    def hand_inward(c, k, to):
        return copy_to(to * plane + p, stage.at[c, k], inward.at[k], i_send.at[k], i_recv.at[k])

    def hand_on(c, k, to):
        return copy_to(to * plane + p, stage.at[c, k], recv.at[c, k], p_send.at[c, k], p_recv.at[c, k])

    steps = chunks
    for_side = ((PLANES - 1 - z, z - 1), (z, z + 1))
    last_of = (half - 1, half)

    colsum[...] = jnp.zeros_like(colsum)

    @pl.loop(0, steps - 1 + 2 * (PLANES - 2))
    def _(step):
        @pl.when(step < steps)
        def _():
            c = chunk_of(step)

            @pl.when(step + AHEAD < steps)
            def _():
                send_weights(step + AHEAD)

            settle(wbuf.at[c], w_recv.at[c])
            partial_products(c)
            for k in range(GRID):
                stage[c, k] = acc[k // 2, :, k % 2 * CHUNK : (k % 2 + 1) * CHUNK].astype(jnp.bfloat16)
            for side in range(2):
                gone, to = for_side[side]

                @pl.when((c // half == side) & (gone == 0))
                def _():
                    for k in range(GRID):
                        hand_on(c, k, to).start()

                @pl.when((c == last_of[side]) & (gone == PLANES - 1))
                def _():
                    for k in range(GRID):
                        hand_inward(c, k, z + (1 - 2 * side)).start()

        for side in range(2):
            gone, to = for_side[side]
            turn = step - 2 * (gone - 1) - jnp.where(gone == PLANES - 1, 2, 0)
            turn = swapped(turn, gone == 1)
            index = jnp.where(turn < 4, turn - 2, turn // 2)
            c = place_of(side, index)
            inner_end = (index == half - 1) & (gone == PLANES - 2)
            due = (turn % 2 == 0) | (turn < 4)
            ready = (gone > 0) & (turn >= 2) & due & (index < half)

            @pl.when(ready & (gone < PLANES - 1) & jnp.logical_not(inner_end))
            def _():
                for k in range(GRID):
                    settle(recv.at[c, k], p_recv.at[c, k])
                    total = stage[c, k].astype(jnp.float32) + recv[c, k].astype(jnp.float32)
                    stage[c, k] = total.astype(jnp.bfloat16)
                    hand_on(c, k, to).start()

            def finish(extra):
                for k in range(GRID):
                    settle(recv.at[c, k], p_recv.at[c, k])
                    residue = stage[c, k].astype(jnp.float32) + recv[c, k].astype(jnp.float32)
                    if extra:
                        settle(inward.at[k], i_recv.at[k])
                        residue += inward[k].astype(jnp.float32)
                    sums = jnp.sum(residue * residue, axis=0, keepdims=True)
                    lanes = pl.ds(pl.multiple_of(c % per * CHUNK, CHUNK), CHUNK)
                    colsum[c // per, k : k + 1, lanes] = sums

            @pl.when(ready & (gone == PLANES - 1) & (index < half - 1))
            def _():
                finish(False)

            @pl.when(ready & inner_end)
            def _():
                finish(True)

    outer = (z == 0) | (z == PLANES - 1)
    inner = jnp.where(z == 0, 1, PLANES - 2)

    def column_copy():
        return copy_to(inner * plane + p, colsum.at[inner], cbuf, c_send, c_recv)

    def total_copy(j):
        return copy_to(z * plane + (p + j) % plane, etile, etiles.at[p], e_send.at[j], e_recv.at[p])

    def line_copy(i):
        return copy_to((z + i) % PLANES * plane + p, ztile, ztiles.at[z], t_send.at[i], t_recv.at[z])

    @pl.when(outer)
    def _():
        column_copy().start()

    total = jnp.zeros((8, 1), jnp.float32)
    for i in range(PLANES):
        total += jnp.sum(colsum[i], axis=1, keepdims=True)
    etile[...] = jnp.broadcast_to(total, (8, LANES))
    for j in range(1, plane):
        total_copy(j).start()
    etiles[p] = etile[...]
    for j in range(1, plane):
        q = (p + j) % plane
        settle(etiles.at[q], e_recv.at[q])
    total = etiles[0]
    for q in range(1, plane):
        total += etiles[q]
    ztile[...] = total
    for i in range(1, PLANES):
        line_copy(i).start()
    ztiles[z] = total

    @pl.when(outer)
    def _():
        col_ref[...] = colsum[z] * (1.0 / tokens)

    @pl.when(jnp.logical_not(outer))
    def _():
        settle(cbuf, c_recv)
        col_ref[...] = (colsum[z] + cbuf[...]) * (1.0 / tokens)

    for i in range(1, PLANES):
        settle(ztiles.at[(z + i) % PLANES], t_recv.at[(z + i) % PLANES])
    total = ztiles[0]
    for i in range(1, PLANES):
        total += ztiles[i]
    on_lane = lax.broadcasted_iota(jnp.int32, (8, LANES), 0) == lax.broadcasted_iota(jnp.int32, (8, LANES), 1)
    err_ref[...] = jnp.sum(jnp.where(on_lane, total, 0.0), axis=0, keepdims=True) * (
        1.0 / (tokens * plane * chunks * CHUNK)
    )

    for i in range(1, PLANES):
        z_copy(i).wait_send()
        mm_copy(i).wait_send()
    for i in range(plane - 1):
        settle(block(0), ab_send.at[i])

    @pl.loop(0, chunks)
    def _(c):
        settle(wbuf.at[0, pl.ds(0, channels - depth), :], w_send.at[c])

        for side in range(2):
            gone, to = for_side[side]

            passed_on = (c // half == side) & (gone < PLANES - 1)
            inner_end = (c == last_of[side]) & (gone == PLANES - 2)

            @pl.when(passed_on & jnp.logical_not(inner_end))
            def _():
                for k in range(GRID):
                    settle(stage.at[c, k], p_send.at[c, k])

    @pl.when(outer)
    def _():
        for k in range(GRID):
            settle(stage.at[0, k], i_send.at[k])
        settle(cbuf, c_send)

    for j in range(1, plane):
        settle(etile, e_send.at[j])
    for i in range(1, PLANES):
        settle(ztile, t_send.at[i])


def shape_results(mean_in, col_in, err_in, mean_ref, col_ref, err_ref):
    mean_ref[...] = mean_in[0, :]
    col_ref[...] = col_in[:GRID, :]
    err_ref[...] = err_in[0, :GRID]


def in_one_kernel(activations, weight):
    n = lax.axis_size("dp")
    own, depth = activations.shape[0], weight.shape[0]
    plane = n // PLANES
    channels, tokens = plane * depth, n * own
    chunks = weight.shape[1] // (plane * CHUNK)
    width = weight.shape[1] // n
    dma, f32, bf16 = pltpu.SemaphoreType.DMA, jnp.float32, jnp.bfloat16
    mean, columns, errors = pl.pallas_call(
        functools.partial(fused_kernel, n),
        out_shape=(
            jax.ShapeDtypeStruct((1, depth), f32),
            jax.ShapeDtypeStruct((8, width), f32),
            jax.ShapeDtypeStruct((1, LANES), f32),
        ),
        in_specs=[pl.BlockSpec(memory_space=pl.ANY)] * 2,
        out_specs=[pl.BlockSpec(memory_space=pltpu.VMEM)] * 3,
        scratch_shapes=[
            pltpu.VMEM((chunks, channels, CHUNK), bf16),
            pltpu.VMEM((tokens, channels), bf16),
            pltpu.VMEM((PLANES, own, channels), bf16),
            pltpu.VMEM((2 * GRID - 2, channels, LANES), f32),
            pltpu.VMEM((1, channels), f32),
            pltpu.VMEM((GRID // 2, BLOCK, 2 * CHUNK), bf16),
            pltpu.VMEM((GRID // 2, tokens, 2 * CHUNK), f32),
            pltpu.VMEM((chunks, GRID, tokens, CHUNK), bf16),
            pltpu.VMEM((chunks, GRID, tokens, CHUNK), bf16),
            pltpu.VMEM((PLANES, 8, width), f32),
            pltpu.VMEM((8, width), f32),
            pltpu.VMEM((8, LANES), f32),
            pltpu.VMEM((PLANES, 8, LANES), f32),
            pltpu.VMEM((8, LANES), f32),
            pltpu.VMEM((plane, 8, LANES), f32),
            pltpu.VMEM((8, LANES), f32),
            pltpu.VMEM((PLANES, 8, LANES), f32),
            pltpu.VMEM((GRID, tokens, CHUNK), bf16),
            dma((chunks,)), dma((chunks,)),
            dma((PLANES,)), dma((PLANES,)),
            dma((plane,)), dma((plane,)),
            dma((PLANES,)), dma((PLANES,)),
            dma((chunks, GRID)), dma((chunks, GRID)),
            dma, dma,
            dma((plane,)), dma((plane,)),
            dma((PLANES,)), dma((PLANES,)),
            dma((GRID,)), dma((GRID,)),
        ],
        compiler_params=pltpu.CompilerParams(
            collective_id=0, has_side_effects=True, vmem_limit_bytes=62 << 20
        ),
    )(activations, weight)
    return pl.pallas_call(
        shape_results,
        out_shape=(
            jax.ShapeDtypeStruct((depth,), f32),
            jax.ShapeDtypeStruct((GRID, width), f32),
            jax.ShapeDtypeStruct((GRID,), f32),
        ),
        in_specs=[pl.BlockSpec(memory_space=pltpu.VMEM)] * 3,
        out_specs=[pl.BlockSpec(memory_space=pltpu.VMEM)] * 3,
    )(mean, columns, errors)


def one_kernel_fits(activations, weight):
    n, tensor = lax.axis_size("dp"), lax.axis_size("tensor")
    if tensor != 1 or n % (2 * PLANES) or n < 4 * PLANES:
        return False
    plane = n // PLANES
    channels, width = plane * weight.shape[0], weight.shape[1]
    aligned = (activations.shape[0] * PLANES) % 16 == 0 and weight.shape[0] % GROUP == 0
    return aligned and channels % BLOCK == 0 and width % (CHUNK * n) == 0


def on_device(activations, weight):
    if one_kernel_fits(activations, weight):
        return in_one_kernel(activations, weight)
    return in_halves(activations, weight)


def solution(mesh):
    placed = (P("dp", "tensor"), P("dp", "tensor"))
    return jax.shard_map(
        on_device,
        mesh=mesh,
        in_specs=placed,
        out_specs=(P("dp"), P(None, ("tensor", "dp")), P()),
        check_vma=False,
    )
```
